32 devices in a mesh: grp: 2 (over y), row: 4 (over z), head: 2 (over x), br: 2 (over core).
Axes of the slice: x: 2, y: 2, z: 4, core: 2. Of those that a mesh axis runs over, the one named last changes fastest.
Arguments:
- pair_acts: float32 [16, 8, 128], P(('grp', 'row', 'head')), parts along dimension 0, may hold values from -6 to 6
- alignment: float32 [64, 8, 256], P(('grp', 'br'), ('row', 'head')), parts along dimension 0, may hold values from -6 to 6
- align_mask: int32 [64, 8], P('grp', ('row', 'head')), parts along dimension 0, may hold values from 0 to 1
- residue_mask: int32 [16], P('grp'), parts along dimension 0, may hold values from 0 to 1, as said below
- align_gain: float32 [256], replicated, may hold values from 0.25 to 1.75
- outer_in: float32 [256, 64], replicated, may hold values from -0.375 to 0.375
- outer_out: float32 [1024, 128], replicated, may hold values from -1 to 1
- tri_gain: float32 [2, 128], replicated, may hold values from 0.25 to 1.75
- tri_in: float32 [2, 128, 4, 128], P(None, None, 'br'), may hold values from -5 to 5
- tri_bias: float32 [2, 128, 4], P(None, None, 'br'), may hold values from -0.5 to 0.5
- tri_out: float32 [2, 4, 32, 128], P(None, 'br'), may hold values from -0.5 to 0.5
- pair_cotangent: float32 [16, 8, 128], P(('grp', 'row', 'head')), parts along dimension 0, may hold values from -6 to 6
Outputs:
- pair_out: float32 [16, 8, 128], P(('grp', 'row', 'head')), parts along dimension 0
- pair_grad: float32 [16, 8, 128], P(('grp', 'row', 'head')), parts along dimension 0
The draws below stay inside these ranges and needn't reach their ends.
There are 2 independent parts, one for each index of `grp`. The reference program is written for one: setup_inputs(seed, part) draws one part's arguments, and reference() takes and returns one part's arrays. A program takes and returns all parts, laid end to end along the dimension named above; an argument that names none is the same for every part. Nothing has to cross between parts.
Inputs may be any that keep to these rules, and one draw needn't show every extreme that they name: `residue_mask`: 1 at residue 0, and 0 at one or more residues; `align_mask`: 1 at every residue of sequence 0 of each part.
All inputs are finite; a program needn't handle non-finite values.
Results may differ from the reference program's by a relative error of at most 0.0003.
Values sent between devices are 32-bit elements; how exact they have to be, the bound alone decides.
No kernel may reach another device: no remote copies, remote signals or barrier semaphores. Data moves between devices by JAX's collectives and lax.ppermute only.
A program may use at most 64 MiB of HBM per device.

```python
import jax
import jax.numpy as jnp
from jax import lax

C = 128
CM = 256
OPC = 32
HEADS = 4
HD = 32
N = 8
S = 32


def draw_align_mask(key, part):
    draws_int = jax.random.randint(key, (S, N), 0, 4)
    leading = jnp.arange(S)[:, None] == 0
    return jnp.where(leading, 1, jnp.minimum(draws_int, 1)).astype(jnp.int32)


def draw_residue_mask(key, part):
    first_key = jax.random.fold_in(key, 11)
    second_key = jax.random.fold_in(key, 23)
    draws_int = jax.random.randint(first_key, (N,), 0, 4)
    dropped = jax.random.randint(second_key, (), 1, N)
    places = jnp.arange(N)
    values = jnp.minimum(draws_int, 1)
    values = jnp.where(places == 0, 1, values)
    values = jnp.where(places == dropped, 0, values)
    return values.astype(jnp.int32)


def draw_tri_in(key, part):
    weights = jax.random.truncated_normal(key, -4.0, 4.0, (2, C, HEADS, 4 * HD), jnp.float32) * C ** (-0.5)
    return weights


def shard_levels(own_key, dims, pieces, smallest, largest):
    def one(axis_at, shards_of):
        draws = jax.random.uniform(jax.random.fold_in(jax.random.fold_in(own_key, 6), axis_at), (shards_of,), jnp.float32, smallest / len(pieces), largest / len(pieces))
        return jnp.repeat(jnp.exp(draws), dims[axis_at] // shards_of).reshape((-1,) + (1,) * (len(dims) - axis_at - 1))

    gain = one(*pieces[0])
    for cut in pieces[1:]:
        gain = gain * one(*cut)
    return gain


def gaussian(own_key, dims, scale, most, split=(), dtype=jnp.bfloat16):
    entries = jax.random.normal(own_key, dims, jnp.float32) * scale
    if len(split) > 0:
        entries = shard_levels(own_key, dims, split, -0.22, 0.18) * entries
    return jnp.clip(entries, min=-most, max=most).astype(dtype)


def setup_inputs(seed: int = 0, part: int = 0) -> dict:
    keys = jax.random.split(jax.random.key(seed), 13)
    own_keys = jax.random.split(jax.random.fold_in(keys[12], part), 13)
    pair_acts = gaussian(own_keys[0], (N, N, C), 1.0, 6.0, ((0, 8),), jnp.float32)
    alignment = gaussian(own_keys[1], (S, N, CM), 1.0, 6.0, ((0, 2), (1, 8)), jnp.float32)
    align_mask = draw_align_mask(jax.random.fold_in(jax.random.fold_in(keys[12], part), 71), part)
    residue_mask = draw_residue_mask(jax.random.fold_in(jax.random.fold_in(keys[12], part), 71), part)
    align_gain = jnp.clip(1.0 + 0.15 * jax.random.normal(keys[4], (CM,), jnp.float32), 0.25, 1.75)
    outer_in = gaussian(keys[5], (CM, 2 * OPC), CM ** -0.5, 0.375, (), jnp.float32)
    outer_out = gaussian(keys[6], (OPC * OPC, C), OPC ** -0.5, 1.0, (), jnp.float32)
    tri_gain = jnp.clip(1.0 + 0.15 * jax.random.normal(keys[7], (2, C), jnp.float32), 0.25, 1.75)
    tri_in = draw_tri_in(jax.random.fold_in(keys[12], 71), part)
    tri_bias = gaussian(keys[9], (2, C, HEADS), C ** -0.5, 0.5, ((2, 2),), jnp.float32)
    tri_out = gaussian(keys[10], (2, HEADS, HD, C), (HEADS * HD) ** -0.5, 0.5, ((1, 2),), jnp.float32)
    pair_cotangent = gaussian(own_keys[11], (N, N, C), 1.0, 6.0, ((0, 8),), jnp.float32)
    return dict(pair_acts=pair_acts, alignment=alignment, align_mask=align_mask, residue_mask=residue_mask, align_gain=align_gain, outer_in=outer_in, outer_out=outer_out, tri_gain=tri_gain, tri_in=tri_in, tri_bias=tri_bias, tri_out=tri_out, pair_cotangent=pair_cotangent)


PRECISE = lax.Precision.HIGHEST
EPSILON = 1e-05
MASK_SHIFT = 1000000000.0

def normalize(values, scales):
    average = lax.optimization_barrier(jnp.mean(values, axis=-1, keepdims=True))
    centred = values - average
    spread = lax.optimization_barrier(jnp.mean(centred * centred, axis=-1, keepdims=True))
    return centred * lax.rsqrt(spread + EPSILON) * scales

def outer_update(alignment, align_mask, align_gain, outer_in, outer_out):
    mask_all = align_mask.astype(jnp.float32)
    normed = normalize(alignment, align_gain)
    projected = jnp.einsum('snc,ck->snk', normed, outer_in, precision=PRECISE)
    left_part = projected[..., :OPC] * mask_all[..., None]
    right_part = projected[..., OPC:] * mask_all[..., None]
    table = outer_out.reshape(OPC, OPC, C)
    mixed_left = jnp.einsum('sip,pqc->siqc', left_part, table, precision=PRECISE)
    summed = jnp.einsum('siqc,sjq->ijc', mixed_left, right_part, precision=PRECISE)
    counts = jnp.einsum('si,sj->ij', mask_all, mask_all, precision=PRECISE)
    return summed / counts[..., None]

def row_attention(rows_in, live, scales, weight_in, weight_bias, weight_out):
    normed = normalize(rows_in, scales)
    projected = jnp.einsum('ijc,chd->ijhd', normed, weight_in, precision=PRECISE)
    bias_full = jnp.einsum('jkc,ch->hjk', normed, weight_bias, precision=PRECISE)
    key_shift = (live - 1.0) * MASK_SHIFT
    scale_factor = HD ** (-0.5)

    def one_row(carried):
        row_proj, row_flag = carried
        queries = row_proj[:, :, :HD]
        key_proj = row_proj[:, :, HD:2 * HD]
        value_proj = row_proj[:, :, 2 * HD:3 * HD]
        gating = row_proj[:, :, 3 * HD:]
        logits = jnp.einsum('jhd,khd->hjk', queries, key_proj, precision=PRECISE) * scale_factor
        logits = logits + bias_full + key_shift
        attention = jax.nn.softmax(logits, axis=-1)
        attended = jnp.einsum('hjk,khd->jhd', attention, value_proj, precision=PRECISE)
        gated_out = jax.nn.sigmoid(gating) * attended
        update = jnp.einsum('jhd,hdc->jc', gated_out, weight_out, precision=PRECISE)
        return update * (row_flag * live)[:, None]
    updates = lax.map(one_row, (projected, live))
    return rows_in + updates

def reference(pair_acts, alignment, align_mask, residue_mask, align_gain, outer_in, outer_out, tri_gain, tri_in, tri_bias, tri_out, pair_cotangent):
    live = residue_mask.astype(jnp.float32)
    outer = outer_update(alignment, align_mask, align_gain, outer_in, outer_out)

    def forward(values):
        pair_one = values + outer
        pair_two = row_attention(pair_one, live, tri_gain[0], tri_in[0], tri_bias[0], tri_out[0])
        turned = row_attention(jnp.swapaxes(pair_two, 0, 1), live, tri_gain[1], tri_in[1], tri_bias[1], tri_out[1])
        return jnp.swapaxes(turned, 0, 1)
    pair_out, pull_back = jax.vjp(forward, pair_acts)
    pair_grad, = pull_back(pair_cotangent)
    return (pair_out, pair_grad)
```

```python
import functools

import jax
import jax.numpy as jnp
from jax import lax
from jax.experimental import pallas as pl
from jax.experimental.pallas import tpu as pltpu
from jax.sharding import PartitionSpec as P

OPC = 32


PRECISE = lax.Precision.HIGHEST
EPSILON = 1e-05
MASK_SHIFT = 1000000000.0


def normalize(values, scales):
    average = jnp.mean(values, axis=-1, keepdims=True)
    centred = values - average
    spread = jnp.mean(centred * centred, axis=-1, keepdims=True)
    return centred * lax.rsqrt(spread + EPSILON) * scales


def core_total(values):
    return lax.psum(values, "br")


def reorient(values):
    turned = jnp.swapaxes(values, 0, 1)
    return lax.all_to_all(turned, ("row", "head"), split_axis=0, concat_axis=1, tiled=True)


def prepare(values, scales, weight_in, weight_bias):
    normed = normalize(values, scales)
    projected = jnp.einsum("ijc,chd->ijhd", normed, weight_in, precision=PRECISE)
    bias_local = jnp.einsum("jkc,ch->hjk", normed, weight_bias, precision=PRECISE)
    return (projected, bias_local)


def attend(projected, bias_full, key_shift, weight_out):
    head_size = projected.shape[-1] // 4
    queries = projected[..., :head_size]
    key_proj = projected[..., head_size : 2 * head_size]
    value_proj = projected[..., 2 * head_size : 3 * head_size]
    gating = projected[..., 3 * head_size :]
    logits = jnp.einsum("ijhd,ikhd->ihjk", queries, key_proj, precision=PRECISE) * head_size ** (
        -0.5
    )
    logits = logits + bias_full[None] + key_shift
    attention = jax.nn.softmax(logits, axis=-1)
    attended = jnp.einsum("ihjk,ikhd->ijhd", attention, value_proj, precision=PRECISE)
    gated_out = jax.nn.sigmoid(gating) * attended
    return jnp.einsum("ijhd,hdc->ijc", gated_out, weight_out, precision=PRECISE)


def tri_forward(rows_in, scales, weight_in, weight_bias, weight_out, key_shift, pair_mask):

    def local_prep(values):
        return prepare(values, scales, weight_in, weight_bias)

    (projected, bias_local), pull_prep = jax.vjp(local_prep, rows_in)
    bias_full = lax.all_gather(bias_local, ("row", "head"), axis=1, tiled=True)

    def local_attend(proj_in, bias_in):
        return attend(proj_in, bias_in, key_shift, weight_out)

    partial_out, pull_attend = jax.vjp(local_attend, projected, bias_full)
    total_out = core_total(partial_out)
    return (rows_in + total_out * pair_mask, (pull_prep, pull_attend))


def tri_backward(grad_out, saved, pair_mask):
    pull_prep, pull_attend = saved
    grad_proj, grad_bias = pull_attend(grad_out * pair_mask)
    grad_local = lax.psum_scatter(grad_bias, ("row", "head"), scatter_dimension=1, tiled=True)
    (grad_rows,) = pull_prep((grad_proj, grad_local))
    return grad_out + core_total(grad_rows)


def body(
    pair_acts,
    alignment,
    align_mask,
    residue_mask,
    align_gain,
    outer_in,
    outer_out,
    tri_gain,
    tri_in,
    tri_bias,
    tri_out,
    pair_cotangent,
):
    row_count = pair_acts.shape[0]
    live = residue_mask.astype(jnp.float32)
    key_shift = (live - 1.0) * MASK_SHIFT
    row_live = lax.dynamic_slice_in_dim(
        live, lax.axis_index(("row", "head")) * row_count, row_count, 0
    )
    pair_mask = row_live[:, None, None] * live[None, :, None]
    seq_count = alignment.shape[0]
    mask_all = align_mask.astype(jnp.float32)
    mask_own = lax.dynamic_slice_in_dim(mask_all, lax.axis_index("br") * seq_count, seq_count, 0)
    normed = normalize(alignment, align_gain)
    projected = jnp.einsum("snc,ck->snk", normed, outer_in, precision=PRECISE)
    left_part = projected[..., :OPC] * mask_own[..., None]
    right_part = jnp.swapaxes(projected[..., OPC:] * mask_own[..., None], 1, 2)
    right_all, mask_cols = (
        lax.all_gather(right_part, ("row", "head"), axis=2, tiled=True),
        lax.all_gather(mask_all, ("row", "head"), axis=1, tiled=True),
    )
    counts = jnp.einsum("si,sj->ij", mask_all, mask_cols, precision=PRECISE)
    table = outer_out.reshape(OPC, OPC, outer_out.shape[-1])
    mixed_left = jnp.einsum("sip,pqc->siqc", left_part, table, precision=PRECISE)
    partial_outer = jnp.einsum("siqc,sqj->ijc", mixed_left, right_all, precision=PRECISE)
    outer_sum = core_total(partial_outer)
    pair_one = pair_acts + outer_sum / counts[..., None]
    pair_two, saved_start = tri_forward(
        pair_one, tri_gain[0], tri_in[0], tri_bias[0], tri_out[0], key_shift, pair_mask
    )
    turned_two = reorient(pair_two)
    turned_three, saved_end = tri_forward(
        turned_two, tri_gain[1], tri_in[1], tri_bias[1], tri_out[1], key_shift, pair_mask
    )
    pair_out = reorient(turned_three)
    grad_turned = reorient(pair_cotangent)
    grad_turned = tri_backward(grad_turned, saved_end, pair_mask)
    grad_two = reorient(grad_turned)
    pair_grad = tri_backward(grad_two, saved_start, pair_mask)
    return (pair_out, pair_grad)


F32 = jnp.float32
BF16 = jnp.bfloat16
LANES = 128
SUBLANES = 8
NN = (((1,), (0,)), ((), ()))
NT = (((1,), (1,)), ((), ()))
TN = (((0,), (0,)), ((), ()))


def split2(values):
    high = values.astype(BF16)
    return high, (values - high.astype(F32)).astype(BF16)


def dot(left, right, dims=NN):
    return lax.dot_general(left, right, dims, preferred_element_type=F32)


def times_stacked(values, stacked):
    high, low = split2(values)
    depth = stacked.shape[0] // 2
    return dot(jnp.concatenate([high, high], axis=1), stacked) + dot(low, stacked[:depth])


def fold(product, rows, columns):
    return product[:rows, :columns] + product[:rows, columns:] + product[rows:, :columns]


def times_stacked_t(values, stacked):
    high, low = split2(values)
    product = dot(jnp.concatenate([high, low], axis=0), stacked, NT)
    return fold(product, values.shape[0], stacked.shape[0] // 2)


def times_beside(values, beside):
    high, low = split2(values)
    product = dot(jnp.concatenate([high, low], axis=0), beside)
    return fold(product, values.shape[0], beside.shape[1] // 2)


def centre(values):
    average = jnp.mean(values, axis=-1, keepdims=True)
    centred = values - average
    scale = lax.rsqrt(jnp.mean(centred * centred, axis=-1, keepdims=True) + EPSILON)
    return centred * scale, scale


def regroup(blocks, width):
    groups = blocks[0].shape[1] // width
    return [
        jnp.concatenate([block[:, g * width : (g + 1) * width] for block in blocks], axis=1)
        for g in range(groups)
    ]


def project_kernel(align_ref, mask_ref, gain_ref, proj_ref, pair_ref, cot_ref, out_ref):
    part = lax.axis_index("br")
    seqs, _, width = align_ref.shape
    opc2 = proj_ref.shape[1]
    rows = seqs // 2
    mask = mask_ref[...].astype(F32)
    sequence = lax.broadcasted_iota(jnp.int32, (mask.shape[0], LANES), 0)
    lane = lax.broadcasted_iota(jnp.int32, (mask.shape[0], LANES), 1)
    own = mask_ref[pl.ds(pl.multiple_of(part * seqs, SUBLANES), seqs), :].astype(F32)
    values = jnp.reshape(align_ref[...], (seqs, width))
    normed, _ = centre(values)
    normed = normed * gain_ref[...]
    high, low = split2(proj_ref[...])
    projected = times_beside(normed, jnp.concatenate([high, low], axis=1)) * own
    out_ref[0:rows, :] = jnp.concatenate([projected[:rows], projected[rows:]], axis=1)
    count = pair_ref.shape[1]
    out_ref[rows : rows + count, :] = jnp.where(part == 0, pair_ref[0], cot_ref[0])
    line = jnp.sum(jnp.where(sequence == lane, mask, 0.0), axis=0, keepdims=True)
    out_ref[rows + count :, :] = jnp.broadcast_to(line, (SUBLANES, LANES))


def weights_kernel(own_in, peer_in, own_bias, peer_bias, own_out, peer_out, in_ref, out_ref):
    first = lax.axis_index("br") == 0
    layers, _, heads, width = own_in.shape
    size = width // 4
    for layer in range(layers):
        blocks, lines, ends = [], [], []
        for half in range(2):
            pick = first if half == 0 else jnp.logical_not(first)
            for h in range(heads):
                blocks.append(jnp.where(pick, own_in[layer, :, h, :], peer_in[layer, :, h, :]))
                bias = jnp.where(pick, own_bias[layer, :, h : h + 1], peer_bias[layer, :, h : h + 1])
                lines.append(jnp.broadcast_to(bias, (bias.shape[0], size)))
                ends.append(jnp.where(pick, own_out[layer, h], peer_out[layer, h]))
        table = jnp.concatenate(regroup(blocks, size) + [jnp.concatenate(lines, axis=1)], axis=1)
        in_ref[layer] = jnp.concatenate(split2(table), axis=0)
        out_ref[layer] = jnp.concatenate(split2(jnp.concatenate(ends, axis=0)), axis=0)


def table_kernel(table_ref, out_ref):
    opc = OPC
    high_low = []
    for q in range(opc):
        rows = table_ref[pl.ds(q, opc, stride=opc), :]
        out_ref[q * opc : (q + 1) * opc, :] = jnp.concatenate(split2(rows), axis=1)


def part_kernel(
    heads, own_ref, peer_ref, live_ref, gain_ref, in_ref, end_ref, table_ref, out_ref, grad_ref,
    mixed, keys, vals, lines, turn, many, more,
):
    me = lax.axis_index(("row", "head"))
    first = lax.axis_index("br") == 0
    n = own_ref.shape[0]
    count = n
    rows = own_ref.shape[1] - count - SUBLANES
    total = n * n
    width = gain_ref.shape[1]
    heads_wide = end_ref.shape[1] // 2
    size = heads_wide // heads

    def taken(start, stop, r, flip):
        slot = jnp.bitwise_xor(me, r)
        mine, other = own_ref[slot, start:stop, :], peer_ref[slot, start:stop, :]
        return jnp.where(first, other, mine) if flip else jnp.where(first, mine, other)

    def transpose_rows(values):
        turn[...] = values
        return jnp.concatenate([turn[pl.ds(j, n, stride=n), :] for j in range(n)], axis=0)

    live = [live_ref[k].astype(F32) for k in range(n)]
    sub = lax.broadcasted_iota(jnp.int32, (n, width), 0)
    live_rows = jnp.zeros((n, width), F32)
    for k in range(n):
        live_rows = jnp.where(sub == k, live[k], live_rows)
    pair_mask = jnp.concatenate([live_rows * live[i] for i in range(n)], axis=0)
    shift = [(live[k] - 1.0) * MASK_SHIFT for k in range(n)]

    lefts, rights = [], []
    for flip in (False, True):
        blocks = [taken(0, rows, r, flip) for r in range(n)]
        pieces = regroup(blocks, OPC)
        lefts += [pieces[0], pieces[2]]
        rights += [pieces[1], pieces[3]]
    left, right = jnp.concatenate(lefts, axis=0), jnp.concatenate(rights, axis=0)
    left_high, left_low = split2(left)
    right_high, right_low = split2(right)
    product = dot(
        jnp.concatenate([right_high, right_high, right_low], axis=0),
        jnp.concatenate([left_high, left_low, left_high], axis=0),
        TN,
    )
    per = LANES // OPC
    chunks = []
    for part in range(n // per):
        mixed[part] = product[:, part * LANES : (part + 1) * LANES]
        lots = []
        for base in range(0, OPC, per):
            lots.append(regroup([mixed[part, pl.ds(base + g, n, stride=OPC), :] for g in range(per)], OPC))
        chunks += [[lot[g] for lot in lots] for g in range(per)]
    spread = jnp.concatenate([jnp.concatenate(c, axis=1) for c in chunks], axis=0)
    outer = times_beside(spread, table_ref[...])
    seen = jnp.concatenate(
        [own_ref[jnp.bitwise_xor(me, r), rows + count : rows + count + 1, :] for r in range(n)], axis=0
    )
    both = jnp.concatenate([seen * seen[i : i + 1] for i in range(n)], axis=0)
    counts = dot(both.astype(BF16), jnp.ones((LANES, width), BF16))
    pair = jnp.concatenate([taken(rows, rows + count, r, False) for r in range(n)], axis=0)
    cot = jnp.concatenate([taken(rows, rows + count, r, True) for r in range(n)], axis=0)
    pair_one = pair + outer / counts

    same = lax.broadcasted_iota(jnp.int32, (heads_wide, heads_wide), 0) // size
    head = lax.broadcasted_iota(jnp.int32, (heads_wide, heads_wide), 1) // size
    ones = jnp.where(same == head, 1.0, 0.0).astype(BF16)
    ones = jnp.concatenate([ones, ones], axis=0)
    factor = size ** (-0.5)

    def head_sums(values):
        return dot(jnp.concatenate(split2(values), axis=1), ones)

    def block(values, i):
        return values[i * n : (i + 1) * n]

    def forward(layer, entry):
        hat, scale = centre(entry)
        projected = times_stacked(hat * gain_ref[layer : layer + 1, :], in_ref[layer])
        q, k, v, gate, bias = [
            projected[:, t * heads_wide : (t + 1) * heads_wide] for t in range(5)
        ]
        q = q * factor
        keys[layer], vals[layer] = k, v
        lines[...] = bias
        biases = [lines[pl.ds(kk, n, stride=n), :] + shift[kk] for kk in range(n)]
        logits = head_sums(
            jnp.concatenate(
                [block(q, i) * keys[layer, i * n + kk : i * n + kk + 1, :] for i in range(n) for kk in range(n)],
                axis=0,
            )
        )
        probs, attended = [], []
        for i in range(n):
            own = [block(logits, i * n + kk) + biases[kk] for kk in range(n)]
            top = own[0]
            for item in own[1:]:
                top = jnp.maximum(top, item)
            own = [jnp.exp(item - top) for item in own]
            whole = own[0]
            for item in own[1:]:
                whole = whole + item
            inverse = 1.0 / whole
            own = [item * inverse for item in own]
            probs.append(own)
            mix = own[0] * vals[layer, i * n : i * n + 1, :]
            for kk in range(1, n):
                mix = mix + own[kk] * vals[layer, i * n + kk : i * n + kk + 1, :]
            attended.append(mix)
        attended = jnp.concatenate(attended, axis=0)
        opened = jax.nn.sigmoid(gate)
        update = times_stacked(opened * attended, end_ref[layer])
        return entry + update * pair_mask, (hat, scale, q, opened, attended, probs)

    def row_sums(scratch):
        whole = scratch[pl.ds(0, total, stride=n), :]
        for j in range(1, n):
            whole = whole + scratch[pl.ds(j, total, stride=n), :]
        return whole

    def backward(layer, grad, saved):
        hat, scale, q, opened, attended, probs = saved
        pulled = times_stacked_t(grad * pair_mask, end_ref[layer])
        d_att = pulled * opened
        d_gate = d_att * attended * (1.0 - opened)
        d_probs = head_sums(
            jnp.concatenate(
                [block(d_att, i) * vals[layer, i * n + kk : i * n + kk + 1, :] for i in range(n) for kk in range(n)],
                axis=0,
            )
        )
        d_q, d_bias = [], [None] * n
        for i in range(n):
            own = [block(d_probs, i * n + kk) for kk in range(n)]
            both_ = [probs[i][kk] * own[kk] for kk in range(n)]
            mean = both_[0]
            for item in both_[1:]:
                mean = mean + item
            piece = None
            for kk in range(n):
                d_logit = both_[kk] - probs[i][kk] * mean
                at = (i * n + kk) * n
                many[at : at + n, :] = d_logit * block(q, i)
                more[at : at + n, :] = probs[i][kk] * block(d_att, i)
                term = d_logit * keys[layer, i * n + kk : i * n + kk + 1, :]
                piece = term if piece is None else piece + term
                d_bias[kk] = d_logit if d_bias[kk] is None else d_bias[kk] + d_logit
            d_q.append(piece)
        d_q = jnp.concatenate(d_q, axis=0) * factor
        d_bias = transpose_rows(jnp.concatenate(d_bias, axis=0) * (1.0 / size))
        d_all = jnp.concatenate([d_q, row_sums(many), row_sums(more), d_gate, d_bias], axis=1)
        d_hat = times_stacked_t(d_all, in_ref[layer]) * gain_ref[layer : layer + 1, :]
        inner = d_hat - jnp.mean(d_hat, axis=-1, keepdims=True)
        inner = inner - hat * jnp.mean(d_hat * hat, axis=-1, keepdims=True)
        return grad + inner * scale

    pair_two, saved_start = forward(0, pair_one)
    turned, saved_end = forward(1, transpose_rows(pair_two))
    turn[...] = turned
    out_ref[0] = turn[pl.ds(me, n, stride=n), :]
    grad = backward(1, transpose_rows(cot), saved_end)
    grad = backward(0, transpose_rows(grad), saved_start)
    turn[...] = grad
    grad_ref[0] = turn[pl.ds(pl.multiple_of(me * n, SUBLANES), n), :]


def spec(space=pltpu.VMEM):
    return pl.BlockSpec(memory_space=space)


def cost(flops):
    return pl.CostEstimate(flops=flops, bytes_accessed=1 << 20, transcendentals=0)


def opposite(count, bit):
    return [(k, k ^ bit) for k in range(count)]


def small_body(
    pair_acts,
    alignment,
    align_mask,
    residue_mask,
    align_gain,
    outer_in,
    outer_out,
    tri_gain,
    tri_in,
    tri_bias,
    tri_out,
    pair_cotangent,
):
    _, n, width = pair_acts.shape
    seqs = alignment.shape[0]
    layers, _, heads, quad = tri_in.shape
    inner = 2 * heads * (quad // 4)
    swap = opposite(2, 1)
    peers = [lax.ppermute(v, "br", swap) for v in (tri_in, tri_bias, tri_out)]
    payload = pl.pallas_call(
        project_kernel,
        out_shape=jax.ShapeDtypeStruct((seqs // 2 + n + SUBLANES, LANES), F32),
        in_specs=[spec()] * 6,
        out_specs=spec(),
        name="project",
    )(alignment, align_mask, align_gain[None], outer_in, pair_acts, pair_cotangent)
    table = pl.pallas_call(
        table_kernel,
        out_shape=jax.ShapeDtypeStruct((outer_out.shape[0], 2 * width), BF16),
        in_specs=[spec()],
        out_specs=spec(),
        cost_estimate=cost(1 << 22),
        name="table",
    )(outer_out)
    in_all, end_all = pl.pallas_call(
        weights_kernel,
        out_shape=(
            jax.ShapeDtypeStruct((layers, 2 * width, 5 * inner), BF16),
            jax.ShapeDtypeStruct((layers, 2 * inner, width), BF16),
        ),
        in_specs=[spec()] * 6,
        out_specs=(spec(), spec()),
        cost_estimate=cost(1 << 22),
        name="weights",
    )(tri_in, peers[0], tri_bias, peers[1], tri_out, peers[2])
    held = payload[None]
    heads_axis, rows_axis = lax.axis_size("head"), lax.axis_size("row")
    for axis, size in (("head", heads_axis), ("row", rows_axis)):
        bit = 1
        while bit < size:
            held = jnp.concatenate([held, lax.ppermute(held, axis, opposite(size, bit))], axis=0)
            bit *= 2
    other = lax.ppermute(held, "br", swap)
    square = n * n
    shape = jax.ShapeDtypeStruct((1, n, width), F32)
    return pl.pallas_call(
        functools.partial(part_kernel, 2 * heads),
        out_shape=(shape, shape),
        in_specs=[spec(), spec(), spec(pltpu.SMEM)] + [spec()] * 4,
        out_specs=(spec(), spec()),
        scratch_shapes=[
            pltpu.VMEM((n * OPC // LANES, n * OPC, LANES), F32),
            pltpu.VMEM((layers, square, inner), F32),
            pltpu.VMEM((layers, square, inner), F32),
            pltpu.VMEM((square, inner), F32),
            pltpu.VMEM((square, width), F32),
            pltpu.VMEM((square * n, inner), F32),
            pltpu.VMEM((square * n, inner), F32),
        ],
        name="part",
    )(held, other, residue_mask, tri_gain, in_all, end_all, table)


def is_small(mesh, residues, seqs, width, inner):
    group = mesh.shape["row"] * mesh.shape["head"]
    powers = all(mesh.shape[a] & (mesh.shape[a] - 1) == 0 for a in ("row", "head"))
    return (
        powers
        and mesh.shape["br"] == 2
        and residues == group == SUBLANES
        and seqs % (2 * 2 * SUBLANES) == 0
        and seqs <= LANES
        and 4 * OPC == width == inner == LANES
    )


def solution(mesh):
    in_specs = (
        P(("grp", "row", "head"), None, None),
        P(("grp", "br"), ("row", "head"), None),
        P("grp", ("row", "head")),
        P("grp"),
        P(),
        P(),
        P(),
        P(),
        P(None, None, "br", None),
        P(None, None, "br"),
        P(None, "br", None, None),
        P(("grp", "row", "head"), None, None),
    )
    out_specs = (P(("grp", "row", "head"), None, None), P(("grp", "row", "head"), None, None))

    def mapped(*args):
        residues, seqs = args[0].shape[1], args[1].shape[0] // mesh.shape["grp"]
        width, inner = args[0].shape[2], args[10].shape[1] * args[10].shape[2]
        chosen = small_body if is_small(mesh, residues, seqs, width, inner) else body
        return jax.shard_map(chosen, mesh=mesh, in_specs=in_specs, out_specs=out_specs, check_vma=False)(*args)

    return mapped
```

```python
import functools

import jax
import jax.numpy as jnp
from jax import lax
from jax.experimental import pallas as pl
from jax.experimental.pallas import tpu as pltpu
from jax.sharding import PartitionSpec as P


OPC = 32


PRECISE = lax.Precision.HIGHEST
EPSILON = 1e-05
MASK_SHIFT = 1000000000.0


def normalize(values, scales):
    average = jnp.mean(values, axis=-1, keepdims=True)
    centred = values - average
    spread = jnp.mean(centred * centred, axis=-1, keepdims=True)
    return centred * lax.rsqrt(spread + EPSILON) * scales


def core_total(values):
    return lax.psum(values, "br")


def reorient(values):
    turned = jnp.swapaxes(values, 0, 1)
    return lax.all_to_all(turned, ("row", "head"), split_axis=0, concat_axis=1, tiled=True)


def prepare(values, scales, weight_in, weight_bias):
    normed = normalize(values, scales)
    projected = jnp.einsum("ijc,chd->ijhd", normed, weight_in, precision=PRECISE)
    bias_local = jnp.einsum("jkc,ch->hjk", normed, weight_bias, precision=PRECISE)
    return (projected, bias_local)


def attend(projected, bias_full, key_shift, weight_out):
    head_size = projected.shape[-1] // 4
    queries = projected[..., :head_size]
    key_proj = projected[..., head_size : 2 * head_size]
    value_proj = projected[..., 2 * head_size : 3 * head_size]
    gating = projected[..., 3 * head_size :]
    logits = jnp.einsum("ijhd,ikhd->ihjk", queries, key_proj, precision=PRECISE) * head_size ** (
        -0.5
    )
    logits = logits + bias_full[None] + key_shift
    attention = jax.nn.softmax(logits, axis=-1)
    attended = jnp.einsum("ihjk,ikhd->ijhd", attention, value_proj, precision=PRECISE)
    gated_out = jax.nn.sigmoid(gating) * attended
    return jnp.einsum("ijhd,hdc->ijc", gated_out, weight_out, precision=PRECISE)


def tri_forward(rows_in, scales, weight_in, weight_bias, weight_out, key_shift, pair_mask):

    def local_prep(values):
        return prepare(values, scales, weight_in, weight_bias)

    (projected, bias_local), pull_prep = jax.vjp(local_prep, rows_in)
    bias_full = lax.all_gather(bias_local, ("row", "head"), axis=1, tiled=True)

    def local_attend(proj_in, bias_in):
        return attend(proj_in, bias_in, key_shift, weight_out)

    partial_out, pull_attend = jax.vjp(local_attend, projected, bias_full)
    total_out = core_total(partial_out)
    return (rows_in + total_out * pair_mask, (pull_prep, pull_attend))


def tri_backward(grad_out, saved, pair_mask):
    pull_prep, pull_attend = saved
    grad_proj, grad_bias = pull_attend(grad_out * pair_mask)
    grad_local = lax.psum_scatter(grad_bias, ("row", "head"), scatter_dimension=1, tiled=True)
    (grad_rows,) = pull_prep((grad_proj, grad_local))
    return grad_out + core_total(grad_rows)


def body(
    pair_acts,
    alignment,
    align_mask,
    residue_mask,
    align_gain,
    outer_in,
    outer_out,
    tri_gain,
    tri_in,
    tri_bias,
    tri_out,
    pair_cotangent,
):
    row_count = pair_acts.shape[0]
    live = residue_mask.astype(jnp.float32)
    key_shift = (live - 1.0) * MASK_SHIFT
    row_live = lax.dynamic_slice_in_dim(
        live, lax.axis_index(("row", "head")) * row_count, row_count, 0
    )
    pair_mask = row_live[:, None, None] * live[None, :, None]
    seq_count = alignment.shape[0]
    mask_all = align_mask.astype(jnp.float32)
    mask_own = lax.dynamic_slice_in_dim(mask_all, lax.axis_index("br") * seq_count, seq_count, 0)
    normed = normalize(alignment, align_gain)
    projected = jnp.einsum("snc,ck->snk", normed, outer_in, precision=PRECISE)
    left_part = projected[..., :OPC] * mask_own[..., None]
    right_part = jnp.swapaxes(projected[..., OPC:] * mask_own[..., None], 1, 2)
    right_all, mask_cols = (
        lax.all_gather(right_part, ("row", "head"), axis=2, tiled=True),
        lax.all_gather(mask_all, ("row", "head"), axis=1, tiled=True),
    )
    counts = jnp.einsum("si,sj->ij", mask_all, mask_cols, precision=PRECISE)
    table = outer_out.reshape(OPC, OPC, outer_out.shape[-1])
    mixed_left = jnp.einsum("sip,pqc->siqc", left_part, table, precision=PRECISE)
    partial_outer = jnp.einsum("siqc,sqj->ijc", mixed_left, right_all, precision=PRECISE)
    outer_sum = core_total(partial_outer)
    pair_one = pair_acts + outer_sum / counts[..., None]
    pair_two, saved_start = tri_forward(
        pair_one, tri_gain[0], tri_in[0], tri_bias[0], tri_out[0], key_shift, pair_mask
    )
    turned_two = reorient(pair_two)
    turned_three, saved_end = tri_forward(
        turned_two, tri_gain[1], tri_in[1], tri_bias[1], tri_out[1], key_shift, pair_mask
    )
    pair_out = reorient(turned_three)
    grad_turned = reorient(pair_cotangent)
    grad_turned = tri_backward(grad_turned, saved_end, pair_mask)
    grad_two = reorient(grad_turned)
    pair_grad = tri_backward(grad_two, saved_start, pair_mask)
    return (pair_out, pair_grad)


F32 = jnp.float32
BF16 = jnp.bfloat16
LANES = 128
SUBLANES = 8
NN = (((1,), (0,)), ((), ()))
NT = (((1,), (1,)), ((), ()))
TN = (((0,), (0,)), ((), ()))


def split2(values):
    high = values.astype(BF16)
    return high, (values - high.astype(F32)).astype(BF16)


def dot(left, right, dims=NN):
    return lax.dot_general(left, right, dims, preferred_element_type=F32)


def times_stacked(values, stacked):
    high, low = split2(values)
    depth = stacked.shape[0] // 2
    return dot(jnp.concatenate([high, high], axis=1), stacked) + dot(low, stacked[:depth])


def fold(product, rows, columns):
    return product[:rows, :columns] + product[:rows, columns:] + product[rows:, :columns]


def times_stacked_t(values, stacked):
    high, low = split2(values)
    product = dot(jnp.concatenate([high, low], axis=0), stacked, NT)
    return fold(product, values.shape[0], stacked.shape[0] // 2)


def times_beside(values, beside):
    high, low = split2(values)
    product = dot(jnp.concatenate([high, low], axis=0), beside)
    return fold(product, values.shape[0], beside.shape[1] // 2)


def centre(values):
    average = jnp.mean(values, axis=-1, keepdims=True)
    centred = values - average
    scale = lax.rsqrt(jnp.mean(centred * centred, axis=-1, keepdims=True) + EPSILON)
    return centred * scale, scale


def regroup(blocks, width):
    groups = blocks[0].shape[1] // width
    return [
        jnp.concatenate([block[:, g * width : (g + 1) * width] for block in blocks], axis=1)
        for g in range(groups)
    ]


def project_kernel(*refs):
    count = (len(refs) - 2) // 2
    sources, out_ref, held, sems = refs[:count], refs[count], refs[count + 1 : -1], refs[-1]
    copies = [
        pltpu.make_async_copy(source, place, sems.at[k])
        for k, (source, place) in enumerate(zip(sources, held))
    ]
    for copy in copies:
        copy.start()
    for copy in copies:
        copy.wait()
    project_part(*held, out_ref)


def project_part(align_ref, mask_ref, gain_ref, proj_ref, pair_ref, cot_ref, out_ref):
    part = lax.axis_index("br")
    seqs, _, width = align_ref.shape
    rows = seqs // 2
    line = mask_ref[...].astype(F32)
    sequence = lax.broadcasted_iota(jnp.int32, (seqs, line.shape[1]), 0) + part * seqs
    lane = lax.broadcasted_iota(jnp.int32, (seqs, line.shape[1]), 1)
    own = jnp.sum(jnp.where(sequence == lane, line, 0.0), axis=1, keepdims=True)
    values = jnp.reshape(align_ref[...], (seqs, width))
    normed, _ = centre(values)
    stacked = jnp.concatenate(split2(proj_ref[...]), axis=0)
    projected = times_stacked_t(normed * gain_ref[...], stacked) * own
    out_ref[0:rows, :] = jnp.concatenate([projected[:rows], projected[rows:]], axis=1)
    count = pair_ref.shape[1]
    out_ref[rows : rows + count, :] = jnp.where(part == 0, pair_ref[0], cot_ref[0])
    rest = jnp.zeros((1, LANES - line.shape[1]), F32)
    line = jnp.concatenate([line, rest], axis=1)
    out_ref[rows + count :, :] = jnp.broadcast_to(line, (SUBLANES, LANES))


def weights_kernel(layer, gain_ref, own_in, peer_in, own_bias, peer_bias, own_out, peer_out, in_ref, out_ref):
    first = lax.axis_index("br") == 0
    heads, width = own_in.shape[2:]
    size = width // 4
    blocks, lines, ends = [], [], []
    for half in range(2):
        pick = first if half == 0 else jnp.logical_not(first)
        for h in range(heads):
            blocks.append(jnp.where(pick, own_in[layer, :, h, :], peer_in[layer, :, h, :]))
            bias = jnp.where(pick, own_bias[layer, h : h + 1, :], peer_bias[layer, h : h + 1, :])
            lines.append(jnp.broadcast_to(bias, (size, bias.shape[1])))
            ends.append(jnp.where(pick, own_out[layer, h], peer_out[layer, h]))
    table = jnp.concatenate(regroup(blocks, size) + [jnp.concatenate(lines, axis=0).T], axis=1)
    gain = gain_ref[layer : layer + 1, :]
    table = table * jnp.broadcast_to(gain, (gain.shape[1], gain.shape[1])).T[:, :1]
    in_ref[...] = jnp.concatenate(split2(table), axis=0)
    out_ref[...] = jnp.concatenate(split2(jnp.concatenate(ends, axis=0)), axis=0)


def table_kernel(table_ref, live_ref, out_ref, rows_ref):
    for q in range(OPC):
        rows = table_ref[pl.ds(q, OPC, stride=OPC), :]
        out_ref[q * OPC : (q + 1) * OPC, :] = jnp.concatenate(split2(rows), axis=1)
    sub = lax.broadcasted_iota(jnp.int32, rows_ref.shape, 0)
    live = jnp.zeros(rows_ref.shape, F32)
    for k in range(rows_ref.shape[0]):
        live = jnp.where(sub == k, live_ref[k].astype(F32), live)
    rows_ref[...] = live


def part_kernel(
    heads, own_ref, peer_ref, live_ref, in_0, end_0, in_1, end_1, table_ref, out_ref, grad_ref,
    mixed, keys, vals, lines, turn, many, more,
):
    me = lax.axis_index(("row", "head"))
    first = lax.axis_index("br") == 0
    n = own_ref.shape[0]
    count = n
    rows = own_ref.shape[1] - count - SUBLANES
    total = n * n
    width = live_ref.shape[1]
    in_ref, end_ref = (in_0, in_1), (end_0, end_1)
    heads_wide = end_0.shape[0] // 2
    size = heads_wide // heads

    def taken(start, stop, r, flip):
        slot = jnp.bitwise_xor(me, r)
        mine, other = own_ref[slot, start:stop, :], peer_ref[slot, start:stop, :]
        return jnp.where(first, other, mine) if flip else jnp.where(first, mine, other)

    def transpose_rows(values):
        turn[...] = values
        return jnp.concatenate([turn[pl.ds(j, n, stride=n), :] for j in range(n)], axis=0)

    live = live_ref[...]
    pair_mask = jnp.concatenate([live * live_ref[i : i + 1, :] for i in range(n)], axis=0)
    shift = [(live_ref[k : k + 1, :] - 1.0) * MASK_SHIFT for k in range(n)]

    lefts, rights = [], []
    for flip in (False, True):
        blocks = [taken(0, rows, r, flip) for r in range(n)]
        pieces = regroup(blocks, OPC)
        lefts += [pieces[0], pieces[2]]
        rights += [pieces[1], pieces[3]]
    left, right = jnp.concatenate(lefts, axis=0), jnp.concatenate(rights, axis=0)
    left_high, left_low = split2(left)
    right_high, right_low = split2(right)
    product = dot(
        jnp.concatenate([right_high, right_high, right_low], axis=0),
        jnp.concatenate([left_high, left_low, left_high], axis=0),
        TN,
    )
    per = LANES // OPC
    chunks = []
    for part in range(n // per):
        mixed[part] = product[:, part * LANES : (part + 1) * LANES]
        lots = []
        for base in range(0, OPC, per):
            lots.append(regroup([mixed[part, pl.ds(base + g, n, stride=OPC), :] for g in range(per)], OPC))
        chunks += [[lot[g] for lot in lots] for g in range(per)]
    spread = jnp.concatenate([jnp.concatenate(c, axis=1) for c in chunks], axis=0)
    outer = times_beside(spread, table_ref[...])
    seen = jnp.concatenate(
        [own_ref[jnp.bitwise_xor(me, r), rows + count : rows + count + 1, :] for r in range(n)], axis=0
    )
    both = jnp.concatenate([seen * seen[i : i + 1] for i in range(n)], axis=0)
    counts = dot(both.astype(BF16), jnp.ones((LANES, width), BF16))
    pair = jnp.concatenate([taken(rows, rows + count, r, False) for r in range(n)], axis=0)
    cot = jnp.concatenate([taken(rows, rows + count, r, True) for r in range(n)], axis=0)
    pair_one = pair + outer / counts

    same = lax.broadcasted_iota(jnp.int32, (heads_wide, heads_wide), 0) // size
    head = lax.broadcasted_iota(jnp.int32, (heads_wide, heads_wide), 1) // size
    ones = jnp.where(same == head, 1.0, 0.0).astype(BF16)
    ones = jnp.concatenate([ones, ones], axis=0)
    factor = size ** (-0.5)

    def head_sums(values):
        return dot(jnp.concatenate(split2(values), axis=1), ones)

    def block(values, i):
        return values[i * n : (i + 1) * n]

    def forward(layer, entry):
        hat, scale = centre(entry)
        projected = times_stacked(hat, in_ref[layer][...])
        q, k, v, gate, bias = [
            projected[:, t * heads_wide : (t + 1) * heads_wide] for t in range(5)
        ]
        q = q * factor
        keys[layer], vals[layer] = k, v
        lines[...] = bias
        biases = [lines[pl.ds(kk, n, stride=n), :] + shift[kk] for kk in range(n)]
        logits = head_sums(
            jnp.concatenate(
                [block(q, i) * keys[layer, i * n + kk : i * n + kk + 1, :] for i in range(n) for kk in range(n)],
                axis=0,
            )
        )
        probs, attended = [], []
        for i in range(n):
            own = [block(logits, i * n + kk) + biases[kk] for kk in range(n)]
            top = own[0]
            for item in own[1:]:
                top = jnp.maximum(top, item)
            own = [jnp.exp(item - top) for item in own]
            whole = own[0]
            for item in own[1:]:
                whole = whole + item
            inverse = 1.0 / whole
            own = [item * inverse for item in own]
            probs.append(own)
            mix = own[0] * vals[layer, i * n : i * n + 1, :]
            for kk in range(1, n):
                mix = mix + own[kk] * vals[layer, i * n + kk : i * n + kk + 1, :]
            attended.append(mix)
        attended = jnp.concatenate(attended, axis=0)
        opened = jax.nn.sigmoid(gate)
        update = times_stacked(opened * attended, end_ref[layer][...])
        return entry + update * pair_mask, (hat, scale, q, opened, attended, probs)

    def row_sums(scratch):
        whole = scratch[pl.ds(0, total, stride=n), :]
        for j in range(1, n):
            whole = whole + scratch[pl.ds(j, total, stride=n), :]
        return whole

    def backward(layer, grad, saved):
        hat, scale, q, opened, attended, probs = saved
        pulled = times_stacked_t(grad * pair_mask, end_ref[layer][...])
        d_att = pulled * opened
        d_gate = d_att * attended * (1.0 - opened)
        d_probs = head_sums(
            jnp.concatenate(
                [block(d_att, i) * vals[layer, i * n + kk : i * n + kk + 1, :] for i in range(n) for kk in range(n)],
                axis=0,
            )
        )
        d_q, d_bias = [], [None] * n
        for i in range(n):
            own = [block(d_probs, i * n + kk) for kk in range(n)]
            both_ = [probs[i][kk] * own[kk] for kk in range(n)]
            mean = both_[0]
            for item in both_[1:]:
                mean = mean + item
            piece = None
            for kk in range(n):
                d_logit = both_[kk] - probs[i][kk] * mean
                at = (i * n + kk) * n
                many[at : at + n, :] = d_logit * block(q, i)
                more[at : at + n, :] = probs[i][kk] * block(d_att, i)
                term = d_logit * keys[layer, i * n + kk : i * n + kk + 1, :]
                piece = term if piece is None else piece + term
                d_bias[kk] = d_logit if d_bias[kk] is None else d_bias[kk] + d_logit
            d_q.append(piece)
        d_q = jnp.concatenate(d_q, axis=0) * factor
        d_bias = transpose_rows(jnp.concatenate(d_bias, axis=0) * (1.0 / size))
        d_all = jnp.concatenate([d_q, row_sums(many), row_sums(more), d_gate, d_bias], axis=1)
        d_hat = times_stacked_t(d_all, in_ref[layer][...])
        inner = d_hat - jnp.mean(d_hat, axis=-1, keepdims=True)
        inner = inner - hat * jnp.mean(d_hat * hat, axis=-1, keepdims=True)
        return grad + inner * scale

    pair_two, saved_start = forward(0, pair_one)
    turned, saved_end = forward(1, transpose_rows(pair_two))
    turn[...] = turned
    out_ref[0] = turn[pl.ds(me, n, stride=n), :]
    grad = backward(1, transpose_rows(cot), saved_end)
    grad = backward(0, transpose_rows(grad), saved_start)
    turn[...] = grad
    grad_ref[0] = turn[pl.ds(pl.multiple_of(me * n, SUBLANES), n), :]


def spec(space=pltpu.VMEM):
    return pl.BlockSpec(memory_space=space)


def cost(flops):
    return pl.CostEstimate(flops=flops, bytes_accessed=1 << 20, transcendentals=0)


def limit(mebibytes):
    return pltpu.CompilerParams(vmem_limit_bytes=mebibytes << 20)


def opposite(count, bit):
    return [(k, k ^ bit) for k in range(count)]


def small_body(*args):
    return gathered(*args)


def gathered(
    pair_acts,
    alignment,
    align_mask,
    residue_mask,
    align_gain,
    outer_in,
    outer_out,
    tri_gain,
    tri_in,
    tri_bias,
    tri_out,
    pair_cotangent,
):
    _, n, width = pair_acts.shape
    seqs = alignment.shape[0]
    layers, _, heads, quad = tri_in.shape
    inner = 2 * heads * (quad // 4)
    swap = opposite(2, 1)
    square = n * n
    bias = jnp.swapaxes(tri_bias, 1, 2)
    firsts = (alignment, align_mask.T, align_gain[None], outer_in.T, pair_acts, pair_cotangent)
    payload = pl.pallas_call(
        project_kernel,
        out_shape=jax.ShapeDtypeStruct((seqs // 2 + n + SUBLANES, LANES), F32),
        in_specs=[spec(pltpu.HBM)] * len(firsts),
        out_specs=spec(),
        scratch_shapes=[pltpu.VMEM(v.shape, v.dtype) for v in firsts]
        + [pltpu.SemaphoreType.DMA((len(firsts),))],
        compiler_params=limit(2),
        name="project",
    )(*[pltpu.with_memory_space_constraint(v, pltpu.HBM) for v in firsts])
    table, live_rows = pl.pallas_call(
        table_kernel,
        out_shape=(
            jax.ShapeDtypeStruct((outer_out.shape[0], 2 * width), BF16),
            jax.ShapeDtypeStruct((n, width), F32),
        ),
        in_specs=[spec(), spec(pltpu.SMEM)],
        out_specs=(spec(), spec()),
        compiler_params=limit(4),
        cost_estimate=cost(1 << 22),
        name="table",
    )(outer_out, residue_mask)
    peers = []
    for value in (tri_in, bias, tri_out):
        peers.append(lax.ppermute(value, "br", swap))
    weights = []
    for layer in range(layers):
        weights += pl.pallas_call(
            functools.partial(weights_kernel, layer),
            out_shape=(
                jax.ShapeDtypeStruct((2 * width, 5 * inner), BF16),
                jax.ShapeDtypeStruct((2 * inner, width), BF16),
            ),
            in_specs=[spec()] * 7,
            out_specs=(spec(), spec()),
            compiler_params=limit(4),
            cost_estimate=cost(1 << 22),
        )(tri_gain, tri_in, peers[0], bias, peers[1], tri_out, peers[2])
    held = payload[None]
    steps = []
    for axis in ("head", "row"):
        bit = 1
        while bit < lax.axis_size(axis):
            steps.append((axis, opposite(lax.axis_size(axis), bit)))
            bit *= 2
    for axis, pairs in steps:
        got = lax.ppermute(held, axis, pairs)
        held = jnp.concatenate([held, got], axis=0)
    other = lax.ppermute(held, "br", swap)
    shape = jax.ShapeDtypeStruct((1, n, width), F32)
    return pl.pallas_call(
        functools.partial(part_kernel, 2 * heads),
        out_shape=(shape, shape),
        in_specs=[spec()] * 8,
        out_specs=(spec(), spec()),
        scratch_shapes=[
            pltpu.VMEM((n * OPC // LANES, n * OPC, LANES), F32),
            pltpu.VMEM((layers, square, inner), F32),
            pltpu.VMEM((layers, square, inner), F32),
            pltpu.VMEM((square, inner), F32),
            pltpu.VMEM((square, width), F32),
            pltpu.VMEM((square * n, inner), F32),
            pltpu.VMEM((square * n, inner), F32),
        ],
        compiler_params=limit(8),
        name="part",
    )(held, other, live_rows, *weights, table)


def is_small(mesh, residues, seqs, width, inner):
    group = mesh.shape["row"] * mesh.shape["head"]
    powers = all(mesh.shape[a] & (mesh.shape[a] - 1) == 0 for a in ("row", "head"))
    return (
        powers
        and mesh.shape["br"] == 2
        and residues == group == SUBLANES
        and seqs % (2 * 2 * SUBLANES) == 0
        and seqs <= LANES
        and 4 * OPC == width == inner == LANES
    )


def solution(mesh):
    in_specs = (
        P(("grp", "row", "head"), None, None),
        P(("grp", "br"), ("row", "head"), None),
        P("grp", ("row", "head")),
        P("grp"),
        P(),
        P(),
        P(),
        P(),
        P(None, None, "br", None),
        P(None, None, "br"),
        P(None, "br", None, None),
        P(("grp", "row", "head"), None, None),
    )
    out_specs = (P(("grp", "row", "head"), None, None), P(("grp", "row", "head"), None, None))

    def mapped(*args):
        residues, seqs = args[0].shape[1], args[1].shape[0] // mesh.shape["grp"]
        width, inner = args[0].shape[2], args[10].shape[1] * args[10].shape[2]
        small = is_small(mesh, residues, seqs, width, inner)
        chosen = small_body if small else body
        step = jax.shard_map(chosen, mesh=mesh, in_specs=in_specs, out_specs=out_specs, check_vma=False)
        return step(*args)

    return mapped
```

```python
import functools

import jax
import jax.numpy as jnp
from jax import lax
from jax.experimental import pallas as pl
from jax.experimental.pallas import tpu as pltpu
from jax.sharding import PartitionSpec as P


OPC = 32


PRECISE = lax.Precision.HIGHEST
EPSILON = 1e-05
MASK_SHIFT = 1000000000.0


def normalize(values, scales):
    average = jnp.mean(values, axis=-1, keepdims=True)
    centred = values - average
    spread = jnp.mean(centred * centred, axis=-1, keepdims=True)
    return centred * lax.rsqrt(spread + EPSILON) * scales


def core_total(values):
    return lax.psum(values, "br")


def reorient(values):
    turned = jnp.swapaxes(values, 0, 1)
    return lax.all_to_all(turned, ("row", "head"), split_axis=0, concat_axis=1, tiled=True)


def prepare(values, scales, weight_in, weight_bias):
    normed = normalize(values, scales)
    projected = jnp.einsum("ijc,chd->ijhd", normed, weight_in, precision=PRECISE)
    bias_local = jnp.einsum("jkc,ch->hjk", normed, weight_bias, precision=PRECISE)
    return (projected, bias_local)


def attend(projected, bias_full, key_shift, weight_out):
    head_size = projected.shape[-1] // 4
    queries = projected[..., :head_size]
    key_proj = projected[..., head_size : 2 * head_size]
    value_proj = projected[..., 2 * head_size : 3 * head_size]
    gating = projected[..., 3 * head_size :]
    logits = jnp.einsum("ijhd,ikhd->ihjk", queries, key_proj, precision=PRECISE) * head_size ** (
        -0.5
    )
    logits = logits + bias_full[None] + key_shift
    attention = jax.nn.softmax(logits, axis=-1)
    attended = jnp.einsum("ihjk,ikhd->ijhd", attention, value_proj, precision=PRECISE)
    gated_out = jax.nn.sigmoid(gating) * attended
    return jnp.einsum("ijhd,hdc->ijc", gated_out, weight_out, precision=PRECISE)


def tri_forward(rows_in, scales, weight_in, weight_bias, weight_out, key_shift, pair_mask):

    def local_prep(values):
        return prepare(values, scales, weight_in, weight_bias)

    (projected, bias_local), pull_prep = jax.vjp(local_prep, rows_in)
    bias_full = lax.all_gather(bias_local, ("row", "head"), axis=1, tiled=True)

    def local_attend(proj_in, bias_in):
        return attend(proj_in, bias_in, key_shift, weight_out)

    partial_out, pull_attend = jax.vjp(local_attend, projected, bias_full)
    total_out = core_total(partial_out)
    return (rows_in + total_out * pair_mask, (pull_prep, pull_attend))


def tri_backward(grad_out, saved, pair_mask):
    pull_prep, pull_attend = saved
    grad_proj, grad_bias = pull_attend(grad_out * pair_mask)
    grad_local = lax.psum_scatter(grad_bias, ("row", "head"), scatter_dimension=1, tiled=True)
    (grad_rows,) = pull_prep((grad_proj, grad_local))
    return grad_out + core_total(grad_rows)


def body(
    pair_acts,
    alignment,
    align_mask,
    residue_mask,
    align_gain,
    outer_in,
    outer_out,
    tri_gain,
    tri_in,
    tri_bias,
    tri_out,
    pair_cotangent,
):
    row_count = pair_acts.shape[0]
    live = residue_mask.astype(jnp.float32)
    key_shift = (live - 1.0) * MASK_SHIFT
    row_live = lax.dynamic_slice_in_dim(
        live, lax.axis_index(("row", "head")) * row_count, row_count, 0
    )
    pair_mask = row_live[:, None, None] * live[None, :, None]
    seq_count = alignment.shape[0]
    mask_all = align_mask.astype(jnp.float32)
    mask_own = lax.dynamic_slice_in_dim(mask_all, lax.axis_index("br") * seq_count, seq_count, 0)
    normed = normalize(alignment, align_gain)
    projected = jnp.einsum("snc,ck->snk", normed, outer_in, precision=PRECISE)
    left_part = projected[..., :OPC] * mask_own[..., None]
    right_part = jnp.swapaxes(projected[..., OPC:] * mask_own[..., None], 1, 2)
    right_all, mask_cols = (
        lax.all_gather(right_part, ("row", "head"), axis=2, tiled=True),
        lax.all_gather(mask_all, ("row", "head"), axis=1, tiled=True),
    )
    counts = jnp.einsum("si,sj->ij", mask_all, mask_cols, precision=PRECISE)
    table = outer_out.reshape(OPC, OPC, outer_out.shape[-1])
    mixed_left = jnp.einsum("sip,pqc->siqc", left_part, table, precision=PRECISE)
    partial_outer = jnp.einsum("siqc,sqj->ijc", mixed_left, right_all, precision=PRECISE)
    outer_sum = core_total(partial_outer)
    pair_one = pair_acts + outer_sum / counts[..., None]
    pair_two, saved_start = tri_forward(
        pair_one, tri_gain[0], tri_in[0], tri_bias[0], tri_out[0], key_shift, pair_mask
    )
    turned_two = reorient(pair_two)
    turned_three, saved_end = tri_forward(
        turned_two, tri_gain[1], tri_in[1], tri_bias[1], tri_out[1], key_shift, pair_mask
    )
    pair_out = reorient(turned_three)
    grad_turned = reorient(pair_cotangent)
    grad_turned = tri_backward(grad_turned, saved_end, pair_mask)
    grad_two = reorient(grad_turned)
    pair_grad = tri_backward(grad_two, saved_start, pair_mask)
    return (pair_out, pair_grad)


F32 = jnp.float32
BF16 = jnp.bfloat16
LANES = 128
SUBLANES = 8
NN = (((1,), (0,)), ((), ()))
NT = (((1,), (1,)), ((), ()))
TN = (((0,), (0,)), ((), ()))


def split2(values):
    high = values.astype(BF16)
    return high, (values - high.astype(F32)).astype(BF16)


def dot(left, right, dims=NN):
    return lax.dot_general(left, right, dims, preferred_element_type=F32)


def times_stacked(values, stacked):
    high, low = split2(values)
    depth = stacked.shape[0] // 2
    return dot(jnp.concatenate([high, high], axis=1), stacked) + dot(low, stacked[:depth])


def fold(product, rows, columns):
    return product[:rows, :columns] + product[:rows, columns:] + product[rows:, :columns]


def times_stacked_t(values, stacked):
    high, low = split2(values)
    product = dot(jnp.concatenate([high, low], axis=0), stacked, NT)
    return fold(product, values.shape[0], stacked.shape[0] // 2)


def times_beside(values, beside):
    high, low = split2(values)
    product = dot(jnp.concatenate([high, low], axis=0), beside)
    return fold(product, values.shape[0], beside.shape[1] // 2)


def centre(values):
    average = jnp.mean(values, axis=-1, keepdims=True)
    centred = values - average
    scale = lax.rsqrt(jnp.mean(centred * centred, axis=-1, keepdims=True) + EPSILON)
    return centred * scale, scale


def regroup(blocks, width):
    groups = blocks[0].shape[1] // width
    return [
        jnp.concatenate([block[:, g * width : (g + 1) * width] for block in blocks], axis=1)
        for g in range(groups)
    ]


def project_kernel(*refs):
    count = (len(refs) - 2) // 2
    sources, out_ref, held, sems = refs[:count], refs[count], refs[count + 1 : -1], refs[-1]
    copies = [
        pltpu.make_async_copy(source, place, sems.at[k])
        for k, (source, place) in enumerate(zip(sources, held))
    ]
    for copy in copies:
        copy.start()
    for copy in copies:
        copy.wait()
    project_part(*held, out_ref)


def project_part(align_ref, mask_ref, gain_ref, proj_ref, pair_ref, cot_ref, out_ref):
    part = lax.axis_index("br")
    seqs, _, width = align_ref.shape
    rows = seqs // 2
    line = mask_ref[...].astype(F32)
    sequence = lax.broadcasted_iota(jnp.int32, (seqs, line.shape[1]), 0) + part * seqs
    lane = lax.broadcasted_iota(jnp.int32, (seqs, line.shape[1]), 1)
    own = jnp.sum(jnp.where(sequence == lane, line, 0.0), axis=1, keepdims=True)
    values = jnp.reshape(align_ref[...], (seqs, width))
    normed, _ = centre(values)
    stacked = jnp.concatenate(split2(proj_ref[...]), axis=0)
    projected = times_stacked_t(normed * gain_ref[...], stacked) * own
    out_ref[0:rows, :] = jnp.concatenate([projected[:rows], projected[rows:]], axis=1)
    count = pair_ref.shape[1]
    out_ref[rows : rows + count, :] = jnp.where(part == 0, pair_ref[0], cot_ref[0])
    rest = jnp.zeros((1, LANES - line.shape[1]), F32)
    line = jnp.concatenate([line, rest], axis=1)
    out_ref[rows + count :, :] = jnp.broadcast_to(line, (SUBLANES, LANES))


def weights_kernel(layer, gain_ref, own_in, peer_in, own_bias, peer_bias, own_out, peer_out, in_ref, out_ref):
    first = lax.axis_index("br") == 0
    heads, width = own_in.shape[2:]
    size = width // 4
    blocks, lines, ends = [], [], []
    for half in range(2):
        pick = first if half == 0 else jnp.logical_not(first)
        for h in range(heads):
            blocks.append(jnp.where(pick, own_in[layer, :, h, :], peer_in[layer, :, h, :]))
            bias = jnp.where(pick, own_bias[layer, h : h + 1, :], peer_bias[layer, h : h + 1, :])
            lines.append(jnp.broadcast_to(bias, (size, bias.shape[1])))
            ends.append(jnp.where(pick, own_out[layer, h], peer_out[layer, h]))
    table = jnp.concatenate(regroup(blocks, size) + [jnp.concatenate(lines, axis=0).T], axis=1)
    gain = gain_ref[layer : layer + 1, :]
    table = table * jnp.broadcast_to(gain, (gain.shape[1], gain.shape[1])).T[:, :1]
    in_ref[...] = jnp.concatenate(split2(table), axis=0)
    out_ref[...] = jnp.concatenate(split2(jnp.concatenate(ends, axis=0)), axis=0)


def table_kernel(table_ref, live_ref, out_ref, rows_ref):
    for q in range(OPC):
        rows = table_ref[pl.ds(q, OPC, stride=OPC), :]
        out_ref[q * OPC : (q + 1) * OPC, :] = jnp.concatenate(split2(rows), axis=1)
    sub = lax.broadcasted_iota(jnp.int32, rows_ref.shape, 0)
    live = jnp.zeros(rows_ref.shape, F32)
    for k in range(rows_ref.shape[0]):
        live = jnp.where(sub == k, live_ref[k].astype(F32), live)
    rows_ref[...] = live


def part_kernel(
    heads, own_ref, peer_ref, live_ref, in_0, end_0, in_1, end_1, table_ref, out_ref, grad_ref,
    mixed, keys, vals, lines, turns, many, more,
):
    me = lax.axis_index(("row", "head"))
    first = lax.axis_index("br") == 0
    n = own_ref.shape[0]
    count = n
    rows = own_ref.shape[1] - count - SUBLANES
    total = n * n
    width = live_ref.shape[1]
    in_ref, end_ref = (in_0, in_1), (end_0, end_1)
    heads_wide = end_0.shape[0] // 2
    size = heads_wide // heads

    def taken(start, stop, r, flip):
        slot = jnp.bitwise_xor(me, r)
        mine, other = own_ref[slot, start:stop, :], peer_ref[slot, start:stop, :]
        return jnp.where(first, other, mine) if flip else jnp.where(first, mine, other)

    def transpose_rows(values, at):
        turn = turns.at[at]
        turn[...] = values
        return jnp.concatenate([turn[pl.ds(j, n, stride=n), :] for j in range(n)], axis=0)

    live = live_ref[...]
    pair_mask = jnp.concatenate([live * live_ref[i : i + 1, :] for i in range(n)], axis=0)
    shift = [(live_ref[k : k + 1, :] - 1.0) * MASK_SHIFT for k in range(n)]

    lefts, rights = [], []
    for flip in (False, True):
        blocks = [taken(0, rows, r, flip) for r in range(n)]
        pieces = regroup(blocks, OPC)
        lefts += [pieces[0], pieces[2]]
        rights += [pieces[1], pieces[3]]
    left, right = jnp.concatenate(lefts, axis=0), jnp.concatenate(rights, axis=0)
    left_high, left_low = split2(left)
    right_high, right_low = split2(right)
    product = dot(
        jnp.concatenate([right_high, right_high, right_low], axis=0),
        jnp.concatenate([left_high, left_low, left_high], axis=0),
        TN,
    )
    per = LANES // OPC
    chunks = []
    for part in range(n // per):
        mixed[part] = product[:, part * LANES : (part + 1) * LANES]
        lots = []
        for base in range(0, OPC, per):
            lots.append(regroup([mixed[part, pl.ds(base + g, n, stride=OPC), :] for g in range(per)], OPC))
        chunks += [[lot[g] for lot in lots] for g in range(per)]
    spread = jnp.concatenate([jnp.concatenate(c, axis=1) for c in chunks], axis=0)
    outer = times_beside(spread, table_ref[...])
    seen = jnp.concatenate(
        [own_ref[jnp.bitwise_xor(me, r), rows + count : rows + count + 1, :] for r in range(n)], axis=0
    )
    both = jnp.concatenate([seen * seen[i : i + 1] for i in range(n)], axis=0)
    counts = dot(both.astype(BF16), jnp.ones((LANES, width), BF16))
    pair = jnp.concatenate([taken(rows, rows + count, r, False) for r in range(n)], axis=0)
    cot = jnp.concatenate([taken(rows, rows + count, r, True) for r in range(n)], axis=0)
    pair_one = pair + outer / counts

    same = lax.broadcasted_iota(jnp.int32, (heads_wide, heads_wide), 0) // size
    head = lax.broadcasted_iota(jnp.int32, (heads_wide, heads_wide), 1) // size
    ones = jnp.where(same == head, 1.0, 0.0).astype(BF16)
    ones = jnp.concatenate([ones, ones], axis=0)
    factor = size ** (-0.5)

    def head_sums(values):
        return dot(jnp.concatenate(split2(values), axis=1), ones)

    def block(values, i):
        return values[i * n : (i + 1) * n]

    def forward(layer, entry):
        hat, scale = centre(entry)
        projected = times_stacked(hat, in_ref[layer][...])
        q, k, v, gate, bias = [
            projected[:, t * heads_wide : (t + 1) * heads_wide] for t in range(5)
        ]
        q = q * factor
        keys[layer], vals[layer] = k, v
        lines[layer] = bias
        biases = [lines[layer, pl.ds(kk, n, stride=n), :] + shift[kk] for kk in range(n)]
        logits = head_sums(
            jnp.concatenate(
                [block(q, i) * keys[layer, i * n + kk : i * n + kk + 1, :] for i in range(n) for kk in range(n)],
                axis=0,
            )
        )
        probs, attended = [], []
        for i in range(n):
            own = [block(logits, i * n + kk) + biases[kk] for kk in range(n)]
            top = own[0]
            for item in own[1:]:
                top = jnp.maximum(top, item)
            own = [jnp.exp(item - top) for item in own]
            whole = own[0]
            for item in own[1:]:
                whole = whole + item
            inverse = 1.0 / whole
            own = [item * inverse for item in own]
            probs.append(own)
            mix = own[0] * vals[layer, i * n : i * n + 1, :]
            for kk in range(1, n):
                mix = mix + own[kk] * vals[layer, i * n + kk : i * n + kk + 1, :]
            attended.append(mix)
        attended = jnp.concatenate(attended, axis=0)
        opened = jax.nn.sigmoid(gate)
        update = times_stacked(opened * attended, end_ref[layer][...])
        return entry + update * pair_mask, (hat, scale, q, opened, attended, probs)

    def row_sums(scratch):
        whole = scratch[pl.ds(0, total, stride=n), :]
        for j in range(1, n):
            whole = whole + scratch[pl.ds(j, total, stride=n), :]
        return whole

    def backward(layer, grad, saved):
        hat, scale, q, opened, attended, probs = saved
        pulled = times_stacked_t(grad * pair_mask, end_ref[layer][...])
        d_att = pulled * opened
        d_gate = d_att * attended * (1.0 - opened)
        d_probs = head_sums(
            jnp.concatenate(
                [block(d_att, i) * vals[layer, i * n + kk : i * n + kk + 1, :] for i in range(n) for kk in range(n)],
                axis=0,
            )
        )
        d_q, d_bias = [], [None] * n
        for i in range(n):
            own = [block(d_probs, i * n + kk) for kk in range(n)]
            both_ = [probs[i][kk] * own[kk] for kk in range(n)]
            mean = both_[0]
            for item in both_[1:]:
                mean = mean + item
            piece = None
            for kk in range(n):
                d_logit = both_[kk] - probs[i][kk] * mean
                at = (i * n + kk) * n
                many[at : at + n, :] = d_logit * block(q, i)
                more[at : at + n, :] = probs[i][kk] * block(d_att, i)
                term = d_logit * keys[layer, i * n + kk : i * n + kk + 1, :]
                piece = term if piece is None else piece + term
                d_bias[kk] = d_logit if d_bias[kk] is None else d_bias[kk] + d_logit
            d_q.append(piece)
        d_q = jnp.concatenate(d_q, axis=0) * factor
        d_bias = transpose_rows(jnp.concatenate(d_bias, axis=0) * (1.0 / size), 5 + layer)
        d_all = jnp.concatenate([d_q, row_sums(many), row_sums(more), d_gate, d_bias], axis=1)
        d_hat = times_stacked_t(d_all, in_ref[layer][...])
        inner = d_hat - jnp.mean(d_hat, axis=-1, keepdims=True)
        inner = inner - hat * jnp.mean(d_hat * hat, axis=-1, keepdims=True)
        return grad + inner * scale

    pair_two, saved_start = forward(0, pair_one)
    turned, saved_end = forward(1, transpose_rows(pair_two, 0))
    turns[3] = turned
    out_ref[0] = turns[3, pl.ds(me, n, stride=n), :]
    grad = backward(1, transpose_rows(cot, 1), saved_end)
    grad = backward(0, transpose_rows(grad, 2), saved_start)
    turns[4] = grad
    grad_ref[0] = turns[4, pl.ds(pl.multiple_of(me * n, SUBLANES), n), :]


def spec(space=pltpu.VMEM):
    return pl.BlockSpec(memory_space=space)


def cost(flops):
    return pl.CostEstimate(flops=flops, bytes_accessed=1 << 20, transcendentals=0)


def limit(mebibytes):
    return pltpu.CompilerParams(vmem_limit_bytes=mebibytes << 20)


def opposite(count, bit):
    return [(k, k ^ bit) for k in range(count)]


def small_body(*args):
    return gathered(*args)


def gathered(
    pair_acts,
    alignment,
    align_mask,
    residue_mask,
    align_gain,
    outer_in,
    outer_out,
    tri_gain,
    tri_in,
    tri_bias,
    tri_out,
    pair_cotangent,
):
    _, n, width = pair_acts.shape
    seqs = alignment.shape[0]
    layers, _, heads, quad = tri_in.shape
    inner = 2 * heads * (quad // 4)
    swap = opposite(2, 1)
    square = n * n
    bias = jnp.swapaxes(tri_bias, 1, 2)
    firsts = (alignment, align_mask.T, align_gain[None], outer_in.T, pair_acts, pair_cotangent)
    payload = pl.pallas_call(
        project_kernel,
        out_shape=jax.ShapeDtypeStruct((seqs // 2 + n + SUBLANES, LANES), F32),
        in_specs=[spec(pltpu.HBM)] * len(firsts),
        out_specs=spec(),
        scratch_shapes=[pltpu.VMEM(v.shape, v.dtype) for v in firsts]
        + [pltpu.SemaphoreType.DMA((len(firsts),))],
        compiler_params=limit(2),
        name="project",
    )(*[pltpu.with_memory_space_constraint(v, pltpu.HBM) for v in firsts])
    table, live_rows = pl.pallas_call(
        table_kernel,
        out_shape=(
            jax.ShapeDtypeStruct((outer_out.shape[0], 2 * width), BF16),
            jax.ShapeDtypeStruct((n, width), F32),
        ),
        in_specs=[spec(), spec(pltpu.SMEM)],
        out_specs=(spec(), spec()),
        compiler_params=limit(4),
        cost_estimate=cost(1 << 22),
        name="table",
    )(outer_out, residue_mask)
    peers = []
    for value in (tri_in, bias, tri_out):
        peers.append(lax.ppermute(value, "br", swap))
    weights = []
    for layer in range(layers):
        weights += pl.pallas_call(
            functools.partial(weights_kernel, layer),
            out_shape=(
                jax.ShapeDtypeStruct((2 * width, 5 * inner), BF16),
                jax.ShapeDtypeStruct((2 * inner, width), BF16),
            ),
            in_specs=[spec()] * 7,
            out_specs=(spec(), spec()),
            compiler_params=limit(4),
            cost_estimate=cost(1 << 22),
        )(tri_gain, tri_in, peers[0], bias, peers[1], tri_out, peers[2])
    held = payload[None]
    steps = []
    for axis in ("head", "row"):
        bit = 1
        while bit < lax.axis_size(axis):
            steps.append((axis, opposite(lax.axis_size(axis), bit)))
            bit *= 2
    for axis, pairs in steps:
        got = lax.ppermute(held, axis, pairs)
        held = jnp.concatenate([held, got], axis=0)
    other = lax.ppermute(held, "br", swap)
    shape = jax.ShapeDtypeStruct((1, n, width), F32)
    return pl.pallas_call(
        functools.partial(part_kernel, 2 * heads),
        out_shape=(shape, shape),
        in_specs=[spec()] * 8,
        out_specs=(spec(), spec()),
        scratch_shapes=[
            pltpu.VMEM((n * OPC // LANES, n * OPC, LANES), F32),
            pltpu.VMEM((layers, square, inner), F32),
            pltpu.VMEM((layers, square, inner), F32),
            pltpu.VMEM((layers, square, inner), F32),
            pltpu.VMEM((5 + layers, square, width), F32),
            pltpu.VMEM((square * n, inner), F32),
            pltpu.VMEM((square * n, inner), F32),
        ],
        compiler_params=limit(8),
        name="part",
    )(held, other, live_rows, *weights, table)


def is_small(mesh, residues, seqs, width, inner):
    group = mesh.shape["row"] * mesh.shape["head"]
    powers = all(mesh.shape[a] & (mesh.shape[a] - 1) == 0 for a in ("row", "head"))
    return (
        powers
        and mesh.shape["br"] == 2
        and residues == group == SUBLANES
        and seqs % (2 * 2 * SUBLANES) == 0
        and seqs <= LANES
        and 4 * OPC == width == inner == LANES
    )


def solution(mesh):
    in_specs = (
        P(("grp", "row", "head"), None, None),
        P(("grp", "br"), ("row", "head"), None),
        P("grp", ("row", "head")),
        P("grp"),
        P(),
        P(),
        P(),
        P(),
        P(None, None, "br", None),
        P(None, None, "br"),
        P(None, "br", None, None),
        P(("grp", "row", "head"), None, None),
    )
    out_specs = (P(("grp", "row", "head"), None, None), P(("grp", "row", "head"), None, None))

    def mapped(*args):
        residues, seqs = args[0].shape[1], args[1].shape[0] // mesh.shape["grp"]
        width, inner = args[0].shape[2], args[10].shape[1] * args[10].shape[2]
        small = is_small(mesh, residues, seqs, width, inner)
        chosen = small_body if small else body
        step = jax.shard_map(chosen, mesh=mesh, in_specs=in_specs, out_specs=out_specs, check_vma=False)
        return step(*args)

    return mapped
```

```python
import functools

import jax
import jax.numpy as jnp
from jax import lax
from jax.experimental import pallas as pl
from jax.experimental.pallas import tpu as pltpu
from jax.sharding import PartitionSpec as P


OPC = 32


PRECISE = lax.Precision.HIGHEST
EPSILON = 1e-05
MASK_SHIFT = 1000000000.0


def normalize(values, scales):
    average = jnp.mean(values, axis=-1, keepdims=True)
    centred = values - average
    spread = jnp.mean(centred * centred, axis=-1, keepdims=True)
    return centred * lax.rsqrt(spread + EPSILON) * scales


def core_total(values):
    return lax.psum(values, "br")


def reorient(values):
    turned = jnp.swapaxes(values, 0, 1)
    return lax.all_to_all(turned, ("row", "head"), split_axis=0, concat_axis=1, tiled=True)


def prepare(values, scales, weight_in, weight_bias):
    normed = normalize(values, scales)
    projected = jnp.einsum("ijc,chd->ijhd", normed, weight_in, precision=PRECISE)
    bias_local = jnp.einsum("jkc,ch->hjk", normed, weight_bias, precision=PRECISE)
    return (projected, bias_local)


def attend(projected, bias_full, key_shift, weight_out):
    head_size = projected.shape[-1] // 4
    queries = projected[..., :head_size]
    key_proj = projected[..., head_size : 2 * head_size]
    value_proj = projected[..., 2 * head_size : 3 * head_size]
    gating = projected[..., 3 * head_size :]
    logits = jnp.einsum("ijhd,ikhd->ihjk", queries, key_proj, precision=PRECISE) * head_size ** (
        -0.5
    )
    logits = logits + bias_full[None] + key_shift
    attention = jax.nn.softmax(logits, axis=-1)
    attended = jnp.einsum("ihjk,ikhd->ijhd", attention, value_proj, precision=PRECISE)
    gated_out = jax.nn.sigmoid(gating) * attended
    return jnp.einsum("ijhd,hdc->ijc", gated_out, weight_out, precision=PRECISE)


def tri_forward(rows_in, scales, weight_in, weight_bias, weight_out, key_shift, pair_mask):

    def local_prep(values):
        return prepare(values, scales, weight_in, weight_bias)

    (projected, bias_local), pull_prep = jax.vjp(local_prep, rows_in)
    bias_full = lax.all_gather(bias_local, ("row", "head"), axis=1, tiled=True)

    def local_attend(proj_in, bias_in):
        return attend(proj_in, bias_in, key_shift, weight_out)

    partial_out, pull_attend = jax.vjp(local_attend, projected, bias_full)
    total_out = core_total(partial_out)
    return (rows_in + total_out * pair_mask, (pull_prep, pull_attend))


def tri_backward(grad_out, saved, pair_mask):
    pull_prep, pull_attend = saved
    grad_proj, grad_bias = pull_attend(grad_out * pair_mask)
    grad_local = lax.psum_scatter(grad_bias, ("row", "head"), scatter_dimension=1, tiled=True)
    (grad_rows,) = pull_prep((grad_proj, grad_local))
    return grad_out + core_total(grad_rows)


def body(
    pair_acts,
    alignment,
    align_mask,
    residue_mask,
    align_gain,
    outer_in,
    outer_out,
    tri_gain,
    tri_in,
    tri_bias,
    tri_out,
    pair_cotangent,
):
    row_count = pair_acts.shape[0]
    live = residue_mask.astype(jnp.float32)
    key_shift = (live - 1.0) * MASK_SHIFT
    row_live = lax.dynamic_slice_in_dim(
        live, lax.axis_index(("row", "head")) * row_count, row_count, 0
    )
    pair_mask = row_live[:, None, None] * live[None, :, None]
    seq_count = alignment.shape[0]
    mask_all = align_mask.astype(jnp.float32)
    mask_own = lax.dynamic_slice_in_dim(mask_all, lax.axis_index("br") * seq_count, seq_count, 0)
    normed = normalize(alignment, align_gain)
    projected = jnp.einsum("snc,ck->snk", normed, outer_in, precision=PRECISE)
    left_part = projected[..., :OPC] * mask_own[..., None]
    right_part = jnp.swapaxes(projected[..., OPC:] * mask_own[..., None], 1, 2)
    right_all, mask_cols = (
        lax.all_gather(right_part, ("row", "head"), axis=2, tiled=True),
        lax.all_gather(mask_all, ("row", "head"), axis=1, tiled=True),
    )
    counts = jnp.einsum("si,sj->ij", mask_all, mask_cols, precision=PRECISE)
    table = outer_out.reshape(OPC, OPC, outer_out.shape[-1])
    mixed_left = jnp.einsum("sip,pqc->siqc", left_part, table, precision=PRECISE)
    partial_outer = jnp.einsum("siqc,sqj->ijc", mixed_left, right_all, precision=PRECISE)
    outer_sum = core_total(partial_outer)
    pair_one = pair_acts + outer_sum / counts[..., None]
    pair_two, saved_start = tri_forward(
        pair_one, tri_gain[0], tri_in[0], tri_bias[0], tri_out[0], key_shift, pair_mask
    )
    turned_two = reorient(pair_two)
    turned_three, saved_end = tri_forward(
        turned_two, tri_gain[1], tri_in[1], tri_bias[1], tri_out[1], key_shift, pair_mask
    )
    pair_out = reorient(turned_three)
    grad_turned = reorient(pair_cotangent)
    grad_turned = tri_backward(grad_turned, saved_end, pair_mask)
    grad_two = reorient(grad_turned)
    pair_grad = tri_backward(grad_two, saved_start, pair_mask)
    return (pair_out, pair_grad)


F32 = jnp.float32
BF16 = jnp.bfloat16
LANES = 128
SUBLANES = 8
NN = (((1,), (0,)), ((), ()))
NT = (((1,), (1,)), ((), ()))
TN = (((0,), (0,)), ((), ()))


def split2(values):
    high = values.astype(BF16)
    return high, (values - high.astype(F32)).astype(BF16)


def dot(left, right, dims=NN):
    return lax.dot_general(left, right, dims, preferred_element_type=F32)


def times_stacked(values, stacked):
    high, low = split2(values)
    depth = stacked.shape[0] // 2
    return dot(jnp.concatenate([high, high], axis=1), stacked) + dot(low, stacked[:depth])


def fold(product, rows, columns):
    return product[:rows, :columns] + product[:rows, columns:] + product[rows:, :columns]


def times_stacked_t(values, stacked):
    high, low = split2(values)
    product = dot(jnp.concatenate([high, low], axis=0), stacked, NT)
    return fold(product, values.shape[0], stacked.shape[0] // 2)


def times_beside(values, beside):
    high, low = split2(values)
    product = dot(jnp.concatenate([high, low], axis=0), beside)
    return fold(product, values.shape[0], beside.shape[1] // 2)


def centre(values):
    average = jnp.mean(values, axis=-1, keepdims=True)
    centred = values - average
    scale = lax.rsqrt(jnp.mean(centred * centred, axis=-1, keepdims=True) + EPSILON)
    return centred * scale, scale


def regroup(blocks, width):
    groups = blocks[0].shape[1] // width
    return [
        jnp.concatenate([block[:, g * width : (g + 1) * width] for block in blocks], axis=1)
        for g in range(groups)
    ]


def project_kernel(*refs):
    count = (len(refs) - 2) // 2
    sources, out_ref, held, sems = refs[:count], refs[count], refs[count + 1 : -1], refs[-1]
    copies = [
        pltpu.make_async_copy(source, place, sems.at[k])
        for k, (source, place) in enumerate(zip(sources, held))
    ]
    for copy in copies:
        copy.start()
    for copy in copies:
        copy.wait()
    project_part(*held, out_ref)


def project_part(align_ref, mask_ref, gain_ref, proj_ref, pair_ref, cot_ref, out_ref):
    part = lax.axis_index("br")
    seqs, _, width = align_ref.shape
    rows = seqs // 2
    line = mask_ref[...].astype(F32)
    sequence = lax.broadcasted_iota(jnp.int32, (seqs, line.shape[1]), 0) + part * seqs
    lane = lax.broadcasted_iota(jnp.int32, (seqs, line.shape[1]), 1)
    own = jnp.sum(jnp.where(sequence == lane, line, 0.0), axis=1, keepdims=True)
    values = jnp.reshape(align_ref[...], (seqs, width))
    normed, _ = centre(values)
    stacked = jnp.concatenate(split2(proj_ref[...]), axis=0)
    projected = times_stacked_t(normed * gain_ref[...], stacked) * own
    out_ref[0:rows, :] = jnp.concatenate([projected[:rows], projected[rows:]], axis=1)
    count = pair_ref.shape[1]
    out_ref[rows : rows + count, :] = jnp.where(part == 0, pair_ref[0], cot_ref[0])
    rest = jnp.zeros((1, LANES - line.shape[1]), F32)
    line = jnp.concatenate([line, rest], axis=1)
    out_ref[rows + count :, :] = jnp.broadcast_to(line, (SUBLANES, LANES))


def weights_kernel(layer, gain_ref, own_in, peer_in, own_bias, peer_bias, own_out, peer_out, in_ref, out_ref):
    first = lax.axis_index("br") == 0
    heads, width = own_in.shape[2:]
    size = width // 4
    blocks, lines, ends = [], [], []
    for half in range(2):
        pick = first if half == 0 else jnp.logical_not(first)
        for h in range(heads):
            blocks.append(jnp.where(pick, own_in[layer, :, h, :], peer_in[layer, :, h, :]))
            bias = jnp.where(pick, own_bias[layer, h : h + 1, :], peer_bias[layer, h : h + 1, :])
            lines.append(jnp.broadcast_to(bias, (size, bias.shape[1])))
            ends.append(jnp.where(pick, own_out[layer, h], peer_out[layer, h]))
    table = jnp.concatenate(regroup(blocks, size) + [jnp.concatenate(lines, axis=0).T], axis=1)
    gain = gain_ref[layer : layer + 1, :]
    table = table * jnp.broadcast_to(gain, (gain.shape[1], gain.shape[1])).T[:, :1]
    in_ref[...] = jnp.concatenate(split2(table), axis=0)
    out_ref[...] = jnp.concatenate(split2(jnp.concatenate(ends, axis=0)), axis=0)


def table_kernel(table_ref, live_ref, out_ref, rows_ref):
    for q in range(OPC):
        rows = table_ref[pl.ds(q, OPC, stride=OPC), :]
        out_ref[q * OPC : (q + 1) * OPC, :] = jnp.concatenate(split2(rows), axis=1)
    sub = lax.broadcasted_iota(jnp.int32, rows_ref.shape, 0)
    live = jnp.zeros(rows_ref.shape, F32)
    for k in range(rows_ref.shape[0]):
        live = jnp.where(sub == k, live_ref[k].astype(F32), live)
    rows_ref[...] = live


def part_kernel(
    heads, own_ref, peer_ref, live_ref, in_0, end_0, in_1, end_1, table_ref, out_ref, grad_ref,
    mixed, keys, vals, lines, turns, many, more,
):
    me = lax.axis_index(("row", "head"))
    n = own_ref.shape[0]
    bits = bits_of(n)
    mine_at = reverse(me, bits)
    part = lax.axis_index("br") ^ parity(me, bits)
    straight = (part == 0, part == 1)
    count = n
    rows = own_ref.shape[1] - count - SUBLANES
    total = n * n
    width = live_ref.shape[1]
    in_ref, end_ref = (in_0, in_1), (end_0, end_1)
    heads_wide = end_0.shape[0] // 2
    size = heads_wide // heads

    def taken(start, stop, r, flip):
        slot = mine_at ^ reverse(r, bits)
        mine, other = own_ref[slot, start:stop, :], peer_ref[slot, start:stop, :]
        pick = straight[parity(r, bits)]
        return jnp.where(pick, other, mine) if flip else jnp.where(pick, mine, other)

    def transpose_rows(values, at):
        turn = turns.at[at]
        turn[...] = values
        return jnp.concatenate([turn[pl.ds(j, n, stride=n), :] for j in range(n)], axis=0)

    live = live_ref[...]
    pair_mask = jnp.concatenate([live * live_ref[i : i + 1, :] for i in range(n)], axis=0)
    shift = [(live_ref[k : k + 1, :] - 1.0) * MASK_SHIFT for k in range(n)]

    lefts, rights = [], []
    for flip in (False, True):
        blocks = [taken(0, rows, r, flip) for r in range(n)]
        pieces = regroup(blocks, OPC)
        lefts += [pieces[0], pieces[2]]
        rights += [pieces[1], pieces[3]]
    left, right = jnp.concatenate(lefts, axis=0), jnp.concatenate(rights, axis=0)
    left_high, left_low = split2(left)
    right_high, right_low = split2(right)
    product = dot(
        jnp.concatenate([right_high, right_high, right_low], axis=0),
        jnp.concatenate([left_high, left_low, left_high], axis=0),
        TN,
    )
    per = LANES // OPC
    chunks = []
    for piece in range(n // per):
        mixed[piece] = product[:, piece * LANES : (piece + 1) * LANES]
        lots = []
        for base in range(0, OPC, per):
            lots.append(regroup([mixed[piece, pl.ds(base + g, n, stride=OPC), :] for g in range(per)], OPC))
        chunks += [[lot[g] for lot in lots] for g in range(per)]
    spread = jnp.concatenate([jnp.concatenate(c, axis=1) for c in chunks], axis=0)
    outer = times_beside(spread, table_ref[...])
    seen = jnp.concatenate(
        [own_ref[mine_at ^ reverse(r, bits), rows + count : rows + count + 1, :] for r in range(n)], axis=0
    )
    both = jnp.concatenate([seen * seen[i : i + 1] for i in range(n)], axis=0)
    counts = dot(both.astype(BF16), jnp.ones((LANES, width), BF16))
    pair = jnp.concatenate([taken(rows, rows + count, r, False) for r in range(n)], axis=0)
    cot = jnp.concatenate([taken(rows, rows + count, r, True) for r in range(n)], axis=0)
    pair_one = pair + outer / counts

    same = lax.broadcasted_iota(jnp.int32, (heads_wide, heads_wide), 0) // size
    head = lax.broadcasted_iota(jnp.int32, (heads_wide, heads_wide), 1) // size
    ones = jnp.where(same == head, 1.0, 0.0).astype(BF16)
    ones = jnp.concatenate([ones, ones], axis=0)
    factor = size ** (-0.5)

    def head_sums(values):
        return dot(jnp.concatenate(split2(values), axis=1), ones)

    def block(values, i):
        return values[i * n : (i + 1) * n]

    def forward(layer, entry):
        hat, scale = centre(entry)
        projected = times_stacked(hat, in_ref[layer][...])
        q, k, v, gate, bias = [
            projected[:, t * heads_wide : (t + 1) * heads_wide] for t in range(5)
        ]
        q = q * factor
        keys[layer], vals[layer] = k, v
        lines[layer] = bias
        biases = [lines[layer, pl.ds(kk, n, stride=n), :] + shift[kk] for kk in range(n)]
        logits = head_sums(
            jnp.concatenate(
                [block(q, i) * keys[layer, i * n + kk : i * n + kk + 1, :] for i in range(n) for kk in range(n)],
                axis=0,
            )
        )
        probs, attended = [], []
        for i in range(n):
            own = [block(logits, i * n + kk) + biases[kk] for kk in range(n)]
            top = own[0]
            for item in own[1:]:
                top = jnp.maximum(top, item)
            own = [jnp.exp(item - top) for item in own]
            whole = own[0]
            for item in own[1:]:
                whole = whole + item
            inverse = 1.0 / whole
            own = [item * inverse for item in own]
            probs.append(own)
            mix = own[0] * vals[layer, i * n : i * n + 1, :]
            for kk in range(1, n):
                mix = mix + own[kk] * vals[layer, i * n + kk : i * n + kk + 1, :]
            attended.append(mix)
        attended = jnp.concatenate(attended, axis=0)
        opened = jax.nn.sigmoid(gate)
        update = times_stacked(opened * attended, end_ref[layer][...])
        return entry + update * pair_mask, (hat, scale, q, opened, attended, probs)

    def row_sums(scratch):
        whole = scratch[pl.ds(0, total, stride=n), :]
        for j in range(1, n):
            whole = whole + scratch[pl.ds(j, total, stride=n), :]
        return whole

    def backward(layer, grad, saved):
        hat, scale, q, opened, attended, probs = saved
        pulled = times_stacked_t(grad * pair_mask, end_ref[layer][...])
        d_att = pulled * opened
        d_gate = d_att * attended * (1.0 - opened)
        d_probs = head_sums(
            jnp.concatenate(
                [block(d_att, i) * vals[layer, i * n + kk : i * n + kk + 1, :] for i in range(n) for kk in range(n)],
                axis=0,
            )
        )
        d_q, d_bias = [], [None] * n
        for i in range(n):
            own = [block(d_probs, i * n + kk) for kk in range(n)]
            both_ = [probs[i][kk] * own[kk] for kk in range(n)]
            mean = both_[0]
            for item in both_[1:]:
                mean = mean + item
            piece = None
            for kk in range(n):
                d_logit = both_[kk] - probs[i][kk] * mean
                at = (i * n + kk) * n
                many[at : at + n, :] = d_logit * block(q, i)
                more[at : at + n, :] = probs[i][kk] * block(d_att, i)
                term = d_logit * keys[layer, i * n + kk : i * n + kk + 1, :]
                piece = term if piece is None else piece + term
                d_bias[kk] = d_logit if d_bias[kk] is None else d_bias[kk] + d_logit
            d_q.append(piece)
        d_q = jnp.concatenate(d_q, axis=0) * factor
        d_bias = transpose_rows(jnp.concatenate(d_bias, axis=0) * (1.0 / size), 5 + layer)
        d_all = jnp.concatenate([d_q, row_sums(many), row_sums(more), d_gate, d_bias], axis=1)
        d_hat = times_stacked_t(d_all, in_ref[layer][...])
        inner = d_hat - jnp.mean(d_hat, axis=-1, keepdims=True)
        inner = inner - hat * jnp.mean(d_hat * hat, axis=-1, keepdims=True)
        return grad + inner * scale

    pair_two, saved_start = forward(0, pair_one)
    turned, saved_end = forward(1, transpose_rows(pair_two, 0))
    turns[3] = turned
    out_ref[0] = turns[3, pl.ds(me, n, stride=n), :]
    grad = backward(1, transpose_rows(cot, 1), saved_end)
    grad = backward(0, transpose_rows(grad, 2), saved_start)
    turns[4] = grad
    grad_ref[0] = turns[4, pl.ds(pl.multiple_of(me * n, SUBLANES), n), :]


def spec(space=pltpu.VMEM):
    return pl.BlockSpec(memory_space=space)


def cost(flops):
    return pl.CostEstimate(flops=flops, bytes_accessed=1 << 20, transcendentals=0)


def limit(mebibytes):
    return pltpu.CompilerParams(vmem_limit_bytes=mebibytes << 20)


def bits_of(count):
    return count.bit_length() - 1


def reverse(index, bits):
    back = 0
    for k in range(bits):
        back = back | (((index >> k) & 1) << (bits - 1 - k))
    return back


def parity(index, bits):
    odd = 0
    for k in range(bits):
        odd = odd ^ ((index >> k) & 1)
    return odd


def opposite(count, bit):
    return [(k, k ^ bit) for k in range(count)]


def small_body(*args):
    return gathered(*args)


def gathered(
    pair_acts,
    alignment,
    align_mask,
    residue_mask,
    align_gain,
    outer_in,
    outer_out,
    tri_gain,
    tri_in,
    tri_bias,
    tri_out,
    pair_cotangent,
):
    _, n, width = pair_acts.shape
    seqs = alignment.shape[0]
    layers, _, heads, quad = tri_in.shape
    inner = 2 * heads * (quad // 4)
    swap = opposite(2, 1)
    square = n * n
    bias = jnp.swapaxes(tri_bias, 1, 2)
    firsts = (alignment, align_mask.T, align_gain[None], outer_in.T, pair_acts, pair_cotangent)
    payload = pl.pallas_call(
        project_kernel,
        out_shape=jax.ShapeDtypeStruct((seqs // 2 + n + SUBLANES, LANES), F32),
        in_specs=[spec(pltpu.HBM)] * len(firsts),
        out_specs=spec(),
        scratch_shapes=[pltpu.VMEM(v.shape, v.dtype) for v in firsts]
        + [pltpu.SemaphoreType.DMA((len(firsts),))],
        compiler_params=limit(2),
        name="project",
    )(*[pltpu.with_memory_space_constraint(v, pltpu.HBM) for v in firsts])
    table, live_rows = pl.pallas_call(
        table_kernel,
        out_shape=(
            jax.ShapeDtypeStruct((outer_out.shape[0], 2 * width), BF16),
            jax.ShapeDtypeStruct((n, width), F32),
        ),
        in_specs=[spec(), spec(pltpu.SMEM)],
        out_specs=(spec(), spec()),
        compiler_params=limit(4),
        cost_estimate=cost(1 << 22),
        name="table",
    )(outer_out, residue_mask)
    peers = []
    for value in (tri_in, bias, tri_out):
        peers.append(lax.ppermute(value, "br", swap))
    weights = []
    for layer in range(layers):
        weights += pl.pallas_call(
            functools.partial(weights_kernel, layer),
            out_shape=(
                jax.ShapeDtypeStruct((2 * width, 5 * inner), BF16),
                jax.ShapeDtypeStruct((2 * inner, width), BF16),
            ),
            in_specs=[spec()] * 7,
            out_specs=(spec(), spec()),
            compiler_params=limit(4),
            cost_estimate=cost(1 << 22),
        )(tri_gain, tri_in, peers[0], bias, peers[1], tri_out, peers[2])
    held = payload[None]
    for at in range(bits_of(n)):
        pairs = opposite(2 * n, (n >> at) | 1)
        got = lax.ppermute(held, ("row", "head", "br"), pairs)
        held = jnp.concatenate([held, got], axis=0)
    other = lax.ppermute(held, "br", swap)
    shape = jax.ShapeDtypeStruct((1, n, width), F32)
    return pl.pallas_call(
        functools.partial(part_kernel, 2 * heads),
        out_shape=(shape, shape),
        in_specs=[spec()] * 8,
        out_specs=(spec(), spec()),
        scratch_shapes=[
            pltpu.VMEM((n * OPC // LANES, n * OPC, LANES), F32),
            pltpu.VMEM((layers, square, inner), F32),
            pltpu.VMEM((layers, square, inner), F32),
            pltpu.VMEM((layers, square, inner), F32),
            pltpu.VMEM((5 + layers, square, width), F32),
            pltpu.VMEM((square * n, inner), F32),
            pltpu.VMEM((square * n, inner), F32),
        ],
        compiler_params=limit(8),
        name="part",
    )(held, other, live_rows, *weights, table)


def is_small(mesh, residues, seqs, width, inner):
    group = mesh.shape["row"] * mesh.shape["head"]
    powers = all(mesh.shape[a] & (mesh.shape[a] - 1) == 0 for a in ("row", "head"))
    return (
        powers
        and mesh.shape["br"] == 2
        and residues == group == SUBLANES
        and seqs % (2 * 2 * SUBLANES) == 0
        and seqs <= LANES
        and 4 * OPC == width == inner == LANES
    )


def solution(mesh):
    in_specs = (
        P(("grp", "row", "head"), None, None),
        P(("grp", "br"), ("row", "head"), None),
        P("grp", ("row", "head")),
        P("grp"),
        P(),
        P(),
        P(),
        P(),
        P(None, None, "br", None),
        P(None, None, "br"),
        P(None, "br", None, None),
        P(("grp", "row", "head"), None, None),
    )
    out_specs = (P(("grp", "row", "head"), None, None), P(("grp", "row", "head"), None, None))

    def mapped(*args):
        residues, seqs = args[0].shape[1], args[1].shape[0] // mesh.shape["grp"]
        width, inner = args[0].shape[2], args[10].shape[1] * args[10].shape[2]
        small = is_small(mesh, residues, seqs, width, inner)
        chosen = small_body if small else body
        step = jax.shard_map(chosen, mesh=mesh, in_specs=in_specs, out_specs=out_specs, check_vma=False)
        return step(*args)

    return mapped
```

```python
import functools

import jax
import jax.numpy as jnp
from jax import lax
from jax.experimental import pallas as pl
from jax.experimental.pallas import tpu as pltpu
from jax.sharding import PartitionSpec as P


OPC = 32


PRECISE = lax.Precision.HIGHEST
EPSILON = 1e-05
MASK_SHIFT = 1000000000.0


def normalize(values, scales):
    average = jnp.mean(values, axis=-1, keepdims=True)
    centred = values - average
    spread = jnp.mean(centred * centred, axis=-1, keepdims=True)
    return centred * lax.rsqrt(spread + EPSILON) * scales


def core_total(values):
    return lax.psum(values, "br")


def reorient(values):
    turned = jnp.swapaxes(values, 0, 1)
    return lax.all_to_all(turned, ("row", "head"), split_axis=0, concat_axis=1, tiled=True)


def prepare(values, scales, weight_in, weight_bias):
    normed = normalize(values, scales)
    projected = jnp.einsum("ijc,chd->ijhd", normed, weight_in, precision=PRECISE)
    bias_local = jnp.einsum("jkc,ch->hjk", normed, weight_bias, precision=PRECISE)
    return (projected, bias_local)


def attend(projected, bias_full, key_shift, weight_out):
    head_size = projected.shape[-1] // 4
    queries = projected[..., :head_size]
    key_proj = projected[..., head_size : 2 * head_size]
    value_proj = projected[..., 2 * head_size : 3 * head_size]
    gating = projected[..., 3 * head_size :]
    logits = jnp.einsum("ijhd,ikhd->ihjk", queries, key_proj, precision=PRECISE) * head_size ** (
        -0.5
    )
    logits = logits + bias_full[None] + key_shift
    attention = jax.nn.softmax(logits, axis=-1)
    attended = jnp.einsum("ihjk,ikhd->ijhd", attention, value_proj, precision=PRECISE)
    gated_out = jax.nn.sigmoid(gating) * attended
    return jnp.einsum("ijhd,hdc->ijc", gated_out, weight_out, precision=PRECISE)


def tri_forward(rows_in, scales, weight_in, weight_bias, weight_out, key_shift, pair_mask):

    def local_prep(values):
        return prepare(values, scales, weight_in, weight_bias)

    (projected, bias_local), pull_prep = jax.vjp(local_prep, rows_in)
    bias_full = lax.all_gather(bias_local, ("row", "head"), axis=1, tiled=True)

    def local_attend(proj_in, bias_in):
        return attend(proj_in, bias_in, key_shift, weight_out)

    partial_out, pull_attend = jax.vjp(local_attend, projected, bias_full)
    total_out = core_total(partial_out)
    return (rows_in + total_out * pair_mask, (pull_prep, pull_attend))


def tri_backward(grad_out, saved, pair_mask):
    pull_prep, pull_attend = saved
    grad_proj, grad_bias = pull_attend(grad_out * pair_mask)
    grad_local = lax.psum_scatter(grad_bias, ("row", "head"), scatter_dimension=1, tiled=True)
    (grad_rows,) = pull_prep((grad_proj, grad_local))
    return grad_out + core_total(grad_rows)


def body(
    pair_acts,
    alignment,
    align_mask,
    residue_mask,
    align_gain,
    outer_in,
    outer_out,
    tri_gain,
    tri_in,
    tri_bias,
    tri_out,
    pair_cotangent,
):
    row_count = pair_acts.shape[0]
    live = residue_mask.astype(jnp.float32)
    key_shift = (live - 1.0) * MASK_SHIFT
    row_live = lax.dynamic_slice_in_dim(
        live, lax.axis_index(("row", "head")) * row_count, row_count, 0
    )
    pair_mask = row_live[:, None, None] * live[None, :, None]
    seq_count = alignment.shape[0]
    mask_all = align_mask.astype(jnp.float32)
    mask_own = lax.dynamic_slice_in_dim(mask_all, lax.axis_index("br") * seq_count, seq_count, 0)
    normed = normalize(alignment, align_gain)
    projected = jnp.einsum("snc,ck->snk", normed, outer_in, precision=PRECISE)
    left_part = projected[..., :OPC] * mask_own[..., None]
    right_part = jnp.swapaxes(projected[..., OPC:] * mask_own[..., None], 1, 2)
    right_all, mask_cols = (
        lax.all_gather(right_part, ("row", "head"), axis=2, tiled=True),
        lax.all_gather(mask_all, ("row", "head"), axis=1, tiled=True),
    )
    counts = jnp.einsum("si,sj->ij", mask_all, mask_cols, precision=PRECISE)
    table = outer_out.reshape(OPC, OPC, outer_out.shape[-1])
    mixed_left = jnp.einsum("sip,pqc->siqc", left_part, table, precision=PRECISE)
    partial_outer = jnp.einsum("siqc,sqj->ijc", mixed_left, right_all, precision=PRECISE)
    outer_sum = core_total(partial_outer)
    pair_one = pair_acts + outer_sum / counts[..., None]
    pair_two, saved_start = tri_forward(
        pair_one, tri_gain[0], tri_in[0], tri_bias[0], tri_out[0], key_shift, pair_mask
    )
    turned_two = reorient(pair_two)
    turned_three, saved_end = tri_forward(
        turned_two, tri_gain[1], tri_in[1], tri_bias[1], tri_out[1], key_shift, pair_mask
    )
    pair_out = reorient(turned_three)
    grad_turned = reorient(pair_cotangent)
    grad_turned = tri_backward(grad_turned, saved_end, pair_mask)
    grad_two = reorient(grad_turned)
    pair_grad = tri_backward(grad_two, saved_start, pair_mask)
    return (pair_out, pair_grad)


F32 = jnp.float32
BF16 = jnp.bfloat16
LANES = 128
SUBLANES = 8
NN = (((1,), (0,)), ((), ()))
NT = (((1,), (1,)), ((), ()))
TN = (((0,), (0,)), ((), ()))


def split2(values):
    high = values.astype(BF16)
    return high, (values - high.astype(F32)).astype(BF16)


def dot(left, right, dims=NN):
    return lax.dot_general(left, right, dims, preferred_element_type=F32)


def times_stacked(values, stacked):
    high, low = split2(values)
    depth = stacked.shape[0] // 2
    return dot(jnp.concatenate([high, high], axis=1), stacked) + dot(low, stacked[:depth])


def fold(product, rows, columns):
    return product[:rows, :columns] + product[:rows, columns:] + product[rows:, :columns]


def times_stacked_t(values, stacked):
    high, low = split2(values)
    product = dot(jnp.concatenate([high, low], axis=0), stacked, NT)
    return fold(product, values.shape[0], stacked.shape[0] // 2)


def times_beside(values, beside):
    high, low = split2(values)
    product = dot(jnp.concatenate([high, low], axis=0), beside)
    return fold(product, values.shape[0], beside.shape[1] // 2)


def centre(values):
    average = jnp.mean(values, axis=-1, keepdims=True)
    centred = values - average
    scale = lax.rsqrt(jnp.mean(centred * centred, axis=-1, keepdims=True) + EPSILON)
    return centred * scale, scale


def regroup(blocks, width):
    groups = blocks[0].shape[1] // width
    return [
        jnp.concatenate([block[:, g * width : (g + 1) * width] for block in blocks], axis=1)
        for g in range(groups)
    ]


def project_kernel(*refs):
    count = (len(refs) - 2) // 2
    sources, out_ref, held, sems = refs[:count], refs[count], refs[count + 1 : -1], refs[-1]
    copies = [
        pltpu.make_async_copy(source, place, sems.at[k])
        for k, (source, place) in enumerate(zip(sources, held))
    ]
    for copy in copies:
        copy.start()
    align_ref, proj_ref, gain_ref, mask_ref, pair_ref, cot_ref = held
    part = lax.axis_index("br")
    seqs, _, width = align_ref.shape
    rows = seqs // 2
    copies[0].wait()
    normed, _ = centre(jnp.reshape(align_ref[...], (seqs, width)))
    copies[1].wait()
    stacked = jnp.concatenate(split2(proj_ref[...]), axis=0)
    copies[2].wait()
    projected = times_stacked_t(normed * gain_ref[...], stacked)
    copies[3].wait()
    line = mask_ref[...].astype(F32)
    sequence = lax.broadcasted_iota(jnp.int32, (seqs, line.shape[1]), 0) + part * seqs
    lane = lax.broadcasted_iota(jnp.int32, (seqs, line.shape[1]), 1)
    own = jnp.sum(jnp.where(sequence == lane, line, 0.0), axis=1, keepdims=True)
    rest = jnp.zeros((1, LANES - line.shape[1]), F32)
    line = jnp.concatenate([line, rest], axis=1)
    count = pair_ref.shape[1]
    out_ref[rows + count :, :] = jnp.broadcast_to(line, (SUBLANES, LANES))
    copies[4].wait()
    copies[5].wait()
    out_ref[rows : rows + count, :] = jnp.where(part == 0, pair_ref[0], cot_ref[0])
    projected = projected * own
    out_ref[0:rows, :] = jnp.concatenate([projected[:rows], projected[rows:]], axis=1)


def weights_kernel(layer, gain_ref, own_in, peer_in, own_bias, peer_bias, own_out, peer_out, in_ref, out_ref):
    first = lax.axis_index("br") == 0
    heads, width = own_in.shape[2:]
    size = width // 4
    blocks, lines, ends = [], [], []
    for half in range(2):
        pick = first if half == 0 else jnp.logical_not(first)
        for h in range(heads):
            blocks.append(jnp.where(pick, own_in[layer, :, h, :], peer_in[layer, :, h, :]))
            bias = jnp.where(pick, own_bias[layer, h : h + 1, :], peer_bias[layer, h : h + 1, :])
            lines.append(jnp.broadcast_to(bias, (size, bias.shape[1])))
            ends.append(jnp.where(pick, own_out[layer, h], peer_out[layer, h]))
    table = jnp.concatenate(regroup(blocks, size) + [jnp.concatenate(lines, axis=0).T], axis=1)
    gain = gain_ref[layer : layer + 1, :]
    table = table * jnp.broadcast_to(gain, (gain.shape[1], gain.shape[1])).T[:, :1]
    in_ref[...] = jnp.concatenate(split2(table), axis=0)
    out_ref[...] = jnp.concatenate(split2(jnp.concatenate(ends, axis=0)), axis=0)


def table_kernel(table_ref, live_ref, out_ref, rows_ref):
    for q in range(OPC):
        rows = table_ref[pl.ds(q, OPC, stride=OPC), :]
        out_ref[q * OPC : (q + 1) * OPC, :] = jnp.concatenate(split2(rows), axis=1)
    sub = lax.broadcasted_iota(jnp.int32, rows_ref.shape, 0)
    live = jnp.zeros(rows_ref.shape, F32)
    for k in range(rows_ref.shape[0]):
        live = jnp.where(sub == k, live_ref[k].astype(F32), live)
    rows_ref[...] = live


def part_kernel(
    heads, own_ref, peer_ref, live_ref, in_0, end_0, in_1, end_1, table_ref, out_ref, grad_ref,
    mixed, keys, vals, lines, turns, many, more,
):
    me = lax.axis_index(("row", "head"))
    n = own_ref.shape[0]
    bits = bits_of(n)
    mine_at = reverse(me, bits)
    part = lax.axis_index("br") ^ parity(me, bits)
    straight = (part == 0, part == 1)
    count = n
    rows = own_ref.shape[1] - count - SUBLANES
    total = n * n
    width = live_ref.shape[1]
    in_ref, end_ref = (in_0, in_1), (end_0, end_1)
    heads_wide = end_0.shape[0] // 2
    size = heads_wide // heads

    def taken(start, stop, r, flip):
        slot = mine_at ^ reverse(r, bits)
        mine, other = own_ref[slot, start:stop, :], peer_ref[slot, start:stop, :]
        pick = straight[parity(r, bits)]
        return jnp.where(pick, other, mine) if flip else jnp.where(pick, mine, other)

    def transpose_rows(values, at):
        turn = turns.at[at]
        turn[...] = values
        return jnp.concatenate([turn[pl.ds(j, n, stride=n), :] for j in range(n)], axis=0)

    live = live_ref[...]
    pair_mask = jnp.concatenate([live * live_ref[i : i + 1, :] for i in range(n)], axis=0)
    shift = [(live_ref[k : k + 1, :] - 1.0) * MASK_SHIFT for k in range(n)]

    lefts, rights = [], []
    for flip in (False, True):
        blocks = [taken(0, rows, r, flip) for r in range(n)]
        pieces = regroup(blocks, OPC)
        lefts += [pieces[0], pieces[2]]
        rights += [pieces[1], pieces[3]]
    left, right = jnp.concatenate(lefts, axis=0), jnp.concatenate(rights, axis=0)
    left_high, left_low = split2(left)
    right_high, right_low = split2(right)
    product = dot(
        jnp.concatenate([right_high, right_high, right_low], axis=0),
        jnp.concatenate([left_high, left_low, left_high], axis=0),
        TN,
    )
    per = LANES // OPC
    chunks = []
    for piece in range(n // per):
        mixed[piece] = product[:, piece * LANES : (piece + 1) * LANES]
        lots = []
        for base in range(0, OPC, per):
            lots.append(regroup([mixed[piece, pl.ds(base + g, n, stride=OPC), :] for g in range(per)], OPC))
        chunks += [[lot[g] for lot in lots] for g in range(per)]
    spread = jnp.concatenate([jnp.concatenate(c, axis=1) for c in chunks], axis=0)
    outer = times_beside(spread, table_ref[...])
    seen = jnp.concatenate(
        [own_ref[mine_at ^ reverse(r, bits), rows + count : rows + count + 1, :] for r in range(n)], axis=0
    )
    both = jnp.concatenate([seen * seen[i : i + 1] for i in range(n)], axis=0)
    counts = dot(both.astype(BF16), jnp.ones((LANES, width), BF16))
    pair = jnp.concatenate([taken(rows, rows + count, r, False) for r in range(n)], axis=0)
    cot = jnp.concatenate([taken(rows, rows + count, r, True) for r in range(n)], axis=0)
    pair_one = pair + outer / counts

    same = lax.broadcasted_iota(jnp.int32, (heads_wide, heads_wide), 0) // size
    head = lax.broadcasted_iota(jnp.int32, (heads_wide, heads_wide), 1) // size
    ones = jnp.where(same == head, 1.0, 0.0).astype(BF16)
    ones = jnp.concatenate([ones, ones], axis=0)
    factor = size ** (-0.5)

    def head_sums(values):
        return dot(jnp.concatenate(split2(values), axis=1), ones)

    def block(values, i):
        return values[i * n : (i + 1) * n]

    def forward(layer, entry, own_entry=None):
        hat, scale = centre(entry)
        wide = 2 * heads_wide
        pair_qk = times_stacked(hat, in_ref[layer][:, :wide])
        pair_vg = times_stacked(hat, in_ref[layer][:, wide : 2 * wide])
        bias = times_stacked(hat, in_ref[layer][:, 2 * wide :])
        q, k = pair_qk[:, :heads_wide], pair_qk[:, heads_wide:]
        v, gate = pair_vg[:, :heads_wide], pair_vg[:, heads_wide:]
        q = q * factor
        keys[layer], vals[layer] = k, v
        lines[layer] = bias
        biases = [lines[layer, pl.ds(kk, n, stride=n), :] + shift[kk] for kk in range(n)]
        logits = head_sums(
            jnp.concatenate(
                [block(q, i) * keys[layer, i * n + kk : i * n + kk + 1, :] for i in range(n) for kk in range(n)],
                axis=0,
            )
        )
        probs, attended = [], []
        for i in range(n):
            own = [block(logits, i * n + kk) + biases[kk] for kk in range(n)]
            top = own[0]
            for item in own[1:]:
                top = jnp.maximum(top, item)
            own = [jnp.exp(item - top) for item in own]
            whole = own[0]
            for item in own[1:]:
                whole = whole + item
            inverse = 1.0 / whole
            own = [item * inverse for item in own]
            probs.append(own)
            mix = own[0] * vals[layer, i * n : i * n + 1, :]
            for kk in range(1, n):
                mix = mix + own[kk] * vals[layer, i * n + kk : i * n + kk + 1, :]
            attended.append(mix)
        attended = jnp.concatenate(attended, axis=0)
        opened = jax.nn.sigmoid(gate)
        gated, mask = opened * attended, pair_mask
        if own_entry is not None:
            turns[3] = gated
            gated, entry = turns[3, pl.ds(me, n, stride=n), :], own_entry
            mask = live * live_ref[pl.ds(me, 1), :]
        update = times_stacked(gated, end_ref[layer][...])
        return entry + update * mask, (hat, scale, q, opened, attended, probs)

    def row_sums(scratch, start, size):
        whole = scratch[pl.ds(start, size, stride=n), :]
        for j in range(1, n):
            whole = whole + scratch[pl.ds(start + j, size, stride=n), :]
        return whole

    def own_rows(values, at):
        turns[at] = values
        return turns[at, pl.ds(pl.multiple_of(me * n, SUBLANES), n), :]

    def backward(layer, grad, saved, own_only):
        hat, scale, q, opened, attended, probs = saved
        pulled = times_stacked_t(grad * pair_mask, end_ref[layer][...])
        d_att = pulled * opened
        d_gate = d_att * attended * (1.0 - opened)
        d_probs = head_sums(
            jnp.concatenate(
                [block(d_att, i) * vals[layer, i * n + kk : i * n + kk + 1, :] for i in range(n) for kk in range(n)],
                axis=0,
            )
        )
        d_q, d_bias = [], [None] * n
        for i in range(n):
            own = [block(d_probs, i * n + kk) for kk in range(n)]
            both_ = [probs[i][kk] * own[kk] for kk in range(n)]
            mean = both_[0]
            for item in both_[1:]:
                mean = mean + item
            piece = None
            for kk in range(n):
                d_logit = both_[kk] - probs[i][kk] * mean
                at = (i * n + kk) * n
                many[at : at + n, :] = d_logit * block(q, i)
                more[at : at + n, :] = probs[i][kk] * block(d_att, i)
                term = d_logit * keys[layer, i * n + kk : i * n + kk + 1, :]
                piece = term if piece is None else piece + term
                d_bias[kk] = d_logit if d_bias[kk] is None else d_bias[kk] + d_logit
            d_q.append(piece)
        d_q = jnp.concatenate(d_q, axis=0) * factor
        d_bias = jnp.concatenate(d_bias, axis=0) * (1.0 / size)
        start, rows_wanted = 0, total
        if own_only:
            turns[5 + layer] = d_bias
            d_bias = turns[5 + layer, pl.ds(me, n, stride=n), :]
            start, rows_wanted = me * n * n, n
            d_q, d_gate = own_rows(d_q, 4), own_rows(d_gate, 7)
            hat, grad = own_rows(hat, 8), own_rows(grad, 9)
            scale = own_rows(jnp.broadcast_to(scale, (total, width)), 10)
        else:
            d_bias = transpose_rows(d_bias, 5 + layer)
        sums = [row_sums(scratch, start, rows_wanted) for scratch in (many, more)]
        wide = 2 * heads_wide
        d_hat = times_stacked_t(jnp.concatenate([sums[1], d_gate], axis=1), in_ref[layer][:, wide : 2 * wide])
        d_hat = d_hat + times_stacked_t(jnp.concatenate([d_q, sums[0]], axis=1), in_ref[layer][:, :wide])
        d_hat = d_hat + times_stacked_t(d_bias, in_ref[layer][:, 2 * wide :])
        inner = d_hat - jnp.mean(d_hat, axis=-1, keepdims=True)
        inner = inner - hat * jnp.mean(d_hat * hat, axis=-1, keepdims=True)
        return grad + inner * scale

    pair_two, saved_start = forward(0, pair_one)
    turned_two = transpose_rows(pair_two, 0)
    own_two = turns[0, pl.ds(pl.multiple_of(me * n, SUBLANES), n), :]
    out_ref[0], saved_end = forward(1, turned_two, own_two)
    grad = backward(1, transpose_rows(cot, 1), saved_end, False)
    grad_ref[0] = backward(0, transpose_rows(grad, 2), saved_start, True)


def spec(space=pltpu.VMEM):
    return pl.BlockSpec(memory_space=space)


def cost(flops):
    return pl.CostEstimate(flops=flops, bytes_accessed=1 << 20, transcendentals=0)


def limit(mebibytes):
    return pltpu.CompilerParams(vmem_limit_bytes=mebibytes << 20)


def bits_of(count):
    return count.bit_length() - 1


def reverse(index, bits):
    back = 0
    for k in range(bits):
        back = back | (((index >> k) & 1) << (bits - 1 - k))
    return back


def parity(index, bits):
    odd = 0
    for k in range(bits):
        odd = odd ^ ((index >> k) & 1)
    return odd


def opposite(count, bit):
    return [(k, k ^ bit) for k in range(count)]


def small_body(*args):
    return gathered(*args)


def gathered(
    pair_acts,
    alignment,
    align_mask,
    residue_mask,
    align_gain,
    outer_in,
    outer_out,
    tri_gain,
    tri_in,
    tri_bias,
    tri_out,
    pair_cotangent,
):
    _, n, width = pair_acts.shape
    seqs = alignment.shape[0]
    layers, _, heads, quad = tri_in.shape
    inner = 2 * heads * (quad // 4)
    swap = opposite(2, 1)
    square = n * n
    bias = jnp.swapaxes(tri_bias, 1, 2)
    firsts = (alignment, outer_in.T, align_gain[None], align_mask.T, pair_acts, pair_cotangent)
    payload = pl.pallas_call(
        project_kernel,
        out_shape=jax.ShapeDtypeStruct((seqs // 2 + n + SUBLANES, LANES), F32),
        in_specs=[spec(pltpu.HBM)] * len(firsts),
        out_specs=spec(),
        scratch_shapes=[pltpu.VMEM(v.shape, v.dtype) for v in firsts]
        + [pltpu.SemaphoreType.DMA((len(firsts),))],
        compiler_params=limit(2),
        name="project",
    )(*[pltpu.with_memory_space_constraint(v, pltpu.HBM) for v in firsts])
    table, live_rows = pl.pallas_call(
        table_kernel,
        out_shape=(
            jax.ShapeDtypeStruct((outer_out.shape[0], 2 * width), BF16),
            jax.ShapeDtypeStruct((n, width), F32),
        ),
        in_specs=[spec(), spec(pltpu.SMEM)],
        out_specs=(spec(), spec()),
        compiler_params=limit(4),
        cost_estimate=cost(1 << 22),
        name="table",
    )(outer_out, residue_mask)
    peers = []
    for value in (tri_in, bias, tri_out):
        peers.append(lax.ppermute(value, "br", swap))
    weights = []
    for layer in range(layers):
        weights += pl.pallas_call(
            functools.partial(weights_kernel, layer),
            out_shape=(
                jax.ShapeDtypeStruct((2 * width, 5 * inner), BF16),
                jax.ShapeDtypeStruct((2 * inner, width), BF16),
            ),
            in_specs=[spec()] * 7,
            out_specs=(spec(), spec()),
            compiler_params=limit(4),
            cost_estimate=cost(1 << 22),
        )(tri_gain, tri_in, peers[0], bias, peers[1], tri_out, peers[2])
    held = payload[None]
    for at in range(bits_of(n)):
        pairs = opposite(2 * n, (n >> at) | 1)
        got = lax.ppermute(held, ("row", "head", "br"), pairs)
        held = jnp.concatenate([held, got], axis=0)
    other = lax.ppermute(held, "br", swap)
    shape = jax.ShapeDtypeStruct((1, n, width), F32)
    return pl.pallas_call(
        functools.partial(part_kernel, 2 * heads),
        out_shape=(shape, shape),
        in_specs=[spec()] * 8,
        out_specs=(spec(), spec()),
        scratch_shapes=[
            pltpu.VMEM((n * OPC // LANES, n * OPC, LANES), F32),
            pltpu.VMEM((layers, square, inner), F32),
            pltpu.VMEM((layers, square, inner), F32),
            pltpu.VMEM((layers, square, inner), F32),
            pltpu.VMEM((9 + layers, square, width), F32),
            pltpu.VMEM((square * n, inner), F32),
            pltpu.VMEM((square * n, inner), F32),
        ],
        compiler_params=limit(8),
        name="part",
    )(held, other, live_rows, *weights, table)


def is_small(mesh, residues, seqs, width, inner):
    group = mesh.shape["row"] * mesh.shape["head"]
    powers = all(mesh.shape[a] & (mesh.shape[a] - 1) == 0 for a in ("row", "head"))
    return (
        powers
        and mesh.shape["br"] == 2
        and residues == group == SUBLANES
        and seqs % (2 * 2 * SUBLANES) == 0
        and seqs <= LANES
        and 4 * OPC == width == inner == LANES
    )


def solution(mesh):
    in_specs = (
        P(("grp", "row", "head"), None, None),
        P(("grp", "br"), ("row", "head"), None),
        P("grp", ("row", "head")),
        P("grp"),
        P(),
        P(),
        P(),
        P(),
        P(None, None, "br", None),
        P(None, None, "br"),
        P(None, "br", None, None),
        P(("grp", "row", "head"), None, None),
    )
    out_specs = (P(("grp", "row", "head"), None, None), P(("grp", "row", "head"), None, None))

    def mapped(*args):
        residues, seqs = args[0].shape[1], args[1].shape[0] // mesh.shape["grp"]
        width, inner = args[0].shape[2], args[10].shape[1] * args[10].shape[2]
        small = is_small(mesh, residues, seqs, width, inner)
        chosen = small_body if small else body
        step = jax.shard_map(chosen, mesh=mesh, in_specs=in_specs, out_specs=out_specs, check_vma=False)
        return step(*args)

    return mapped
```

```python
import functools

import jax
import jax.numpy as jnp
from jax import lax
from jax.experimental import pallas as pl
from jax.experimental.pallas import tpu as pltpu
from jax.sharding import PartitionSpec as P


OPC = 32


PRECISE = lax.Precision.HIGHEST
EPSILON = 1e-05
MASK_SHIFT = 1000000000.0


def normalize(values, scales):
    average = jnp.mean(values, axis=-1, keepdims=True)
    centred = values - average
    spread = jnp.mean(centred * centred, axis=-1, keepdims=True)
    return centred * lax.rsqrt(spread + EPSILON) * scales


def core_total(values):
    return lax.psum(values, "br")


def reorient(values):
    turned = jnp.swapaxes(values, 0, 1)
    return lax.all_to_all(turned, ("row", "head"), split_axis=0, concat_axis=1, tiled=True)


def prepare(values, scales, weight_in, weight_bias):
    normed = normalize(values, scales)
    projected = jnp.einsum("ijc,chd->ijhd", normed, weight_in, precision=PRECISE)
    bias_local = jnp.einsum("jkc,ch->hjk", normed, weight_bias, precision=PRECISE)
    return (projected, bias_local)


def attend(projected, bias_full, key_shift, weight_out):
    head_size = projected.shape[-1] // 4
    queries = projected[..., :head_size]
    key_proj = projected[..., head_size : 2 * head_size]
    value_proj = projected[..., 2 * head_size : 3 * head_size]
    gating = projected[..., 3 * head_size :]
    logits = jnp.einsum("ijhd,ikhd->ihjk", queries, key_proj, precision=PRECISE) * head_size ** (
        -0.5
    )
    logits = logits + bias_full[None] + key_shift
    attention = jax.nn.softmax(logits, axis=-1)
    attended = jnp.einsum("ihjk,ikhd->ijhd", attention, value_proj, precision=PRECISE)
    gated_out = jax.nn.sigmoid(gating) * attended
    return jnp.einsum("ijhd,hdc->ijc", gated_out, weight_out, precision=PRECISE)


def tri_forward(rows_in, scales, weight_in, weight_bias, weight_out, key_shift, pair_mask):

    def local_prep(values):
        return prepare(values, scales, weight_in, weight_bias)

    (projected, bias_local), pull_prep = jax.vjp(local_prep, rows_in)
    bias_full = lax.all_gather(bias_local, ("row", "head"), axis=1, tiled=True)

    def local_attend(proj_in, bias_in):
        return attend(proj_in, bias_in, key_shift, weight_out)

    partial_out, pull_attend = jax.vjp(local_attend, projected, bias_full)
    total_out = core_total(partial_out)
    return (rows_in + total_out * pair_mask, (pull_prep, pull_attend))


def tri_backward(grad_out, saved, pair_mask):
    pull_prep, pull_attend = saved
    grad_proj, grad_bias = pull_attend(grad_out * pair_mask)
    grad_local = lax.psum_scatter(grad_bias, ("row", "head"), scatter_dimension=1, tiled=True)
    (grad_rows,) = pull_prep((grad_proj, grad_local))
    return grad_out + core_total(grad_rows)


def body(
    pair_acts,
    alignment,
    align_mask,
    residue_mask,
    align_gain,
    outer_in,
    outer_out,
    tri_gain,
    tri_in,
    tri_bias,
    tri_out,
    pair_cotangent,
):
    row_count = pair_acts.shape[0]
    live = residue_mask.astype(jnp.float32)
    key_shift = (live - 1.0) * MASK_SHIFT
    row_live = lax.dynamic_slice_in_dim(
        live, lax.axis_index(("row", "head")) * row_count, row_count, 0
    )
    pair_mask = row_live[:, None, None] * live[None, :, None]
    seq_count = alignment.shape[0]
    mask_all = align_mask.astype(jnp.float32)
    mask_own = lax.dynamic_slice_in_dim(mask_all, lax.axis_index("br") * seq_count, seq_count, 0)
    normed = normalize(alignment, align_gain)
    projected = jnp.einsum("snc,ck->snk", normed, outer_in, precision=PRECISE)
    left_part = projected[..., :OPC] * mask_own[..., None]
    right_part = jnp.swapaxes(projected[..., OPC:] * mask_own[..., None], 1, 2)
    right_all, mask_cols = (
        lax.all_gather(right_part, ("row", "head"), axis=2, tiled=True),
        lax.all_gather(mask_all, ("row", "head"), axis=1, tiled=True),
    )
    counts = jnp.einsum("si,sj->ij", mask_all, mask_cols, precision=PRECISE)
    table = outer_out.reshape(OPC, OPC, outer_out.shape[-1])
    mixed_left = jnp.einsum("sip,pqc->siqc", left_part, table, precision=PRECISE)
    partial_outer = jnp.einsum("siqc,sqj->ijc", mixed_left, right_all, precision=PRECISE)
    outer_sum = core_total(partial_outer)
    pair_one = pair_acts + outer_sum / counts[..., None]
    pair_two, saved_start = tri_forward(
        pair_one, tri_gain[0], tri_in[0], tri_bias[0], tri_out[0], key_shift, pair_mask
    )
    turned_two = reorient(pair_two)
    turned_three, saved_end = tri_forward(
        turned_two, tri_gain[1], tri_in[1], tri_bias[1], tri_out[1], key_shift, pair_mask
    )
    pair_out = reorient(turned_three)
    grad_turned = reorient(pair_cotangent)
    grad_turned = tri_backward(grad_turned, saved_end, pair_mask)
    grad_two = reorient(grad_turned)
    pair_grad = tri_backward(grad_two, saved_start, pair_mask)
    return (pair_out, pair_grad)


F32 = jnp.float32
BF16 = jnp.bfloat16
LANES = 128
SUBLANES = 8
NN = (((1,), (0,)), ((), ()))
NT = (((1,), (1,)), ((), ()))
TN = (((0,), (0,)), ((), ()))


def split2(values):
    high = values.astype(BF16)
    return high, (values - high.astype(F32)).astype(BF16)


def dot(left, right, dims=NN):
    return lax.dot_general(left, right, dims, preferred_element_type=F32)


def times_stacked(values, stacked):
    high, low = split2(values)
    depth = stacked.shape[0] // 2
    return dot(jnp.concatenate([high, high], axis=1), stacked) + dot(low, stacked[:depth])


def fold(product, rows, columns):
    return product[:rows, :columns] + product[:rows, columns:] + product[rows:, :columns]


def times_stacked_t(values, stacked):
    high, low = split2(values)
    product = dot(jnp.concatenate([high, low], axis=0), stacked, NT)
    return fold(product, values.shape[0], stacked.shape[0] // 2)


def times_beside(values, beside):
    high, low = split2(values)
    product = dot(jnp.concatenate([high, low], axis=0), beside)
    return fold(product, values.shape[0], beside.shape[1] // 2)


def centre(values):
    average = jnp.mean(values, axis=-1, keepdims=True)
    centred = values - average
    scale = lax.rsqrt(jnp.mean(centred * centred, axis=-1, keepdims=True) + EPSILON)
    return centred, scale


def regroup(blocks, width):
    groups = blocks[0].shape[1] // width
    return [
        jnp.concatenate([block[:, g * width : (g + 1) * width] for block in blocks], axis=1)
        for g in range(groups)
    ]


def project_kernel(*refs):
    count = (len(refs) - 2) // 2
    sources, out_ref, held, sems = refs[:count], refs[count], refs[count + 1 : -1], refs[-1]
    copies = [
        pltpu.make_async_copy(source, place, sems.at[k])
        for k, (source, place) in enumerate(zip(sources, held))
    ]
    for copy in copies:
        copy.start()
    align_ref, proj_ref, gain_ref, mask_ref, pair_ref, cot_ref = held
    part = lax.axis_index("br")
    seqs, _, width = align_ref.shape
    rows = seqs // 2
    copies[0].wait()
    centred, scale = centre(jnp.reshape(align_ref[...], (seqs, width)))
    normed = centred * scale
    copies[1].wait()
    stacked = jnp.concatenate(split2(proj_ref[...]), axis=0)
    copies[2].wait()
    projected = times_stacked_t(normed * gain_ref[...], stacked)
    copies[3].wait()
    line = mask_ref[...].astype(F32)
    sequence = lax.broadcasted_iota(jnp.int32, (seqs, line.shape[1]), 0) + part * seqs
    lane = lax.broadcasted_iota(jnp.int32, (seqs, line.shape[1]), 1)
    own = jnp.sum(jnp.where(sequence == lane, line, 0.0), axis=1, keepdims=True)
    rest = jnp.zeros((1, LANES - line.shape[1]), F32)
    line = jnp.concatenate([line, rest], axis=1)
    count = pair_ref.shape[1]
    out_ref[rows + count :, :] = jnp.broadcast_to(line, (SUBLANES, LANES))
    copies[4].wait()
    copies[5].wait()
    out_ref[rows : rows + count, :] = jnp.where(part == 0, pair_ref[0], cot_ref[0])
    projected = projected * own
    out_ref[0:rows, :] = jnp.concatenate([projected[:rows], projected[rows:]], axis=1)


def weights_kernel(layer, gain_ref, own_in, peer_in, own_bias, peer_bias, own_out, peer_out, in_ref, out_ref, *both_ref):
    first = lax.axis_index("br") == 0
    heads, width = own_in.shape[2:]
    size = width // 4
    blocks, lines, ends, before = [], [], [], []
    for half in range(2):
        pick = first if half == 0 else jnp.logical_not(first)
        for h in range(heads):
            blocks.append(jnp.where(pick, own_in[layer, :, h, :], peer_in[layer, :, h, :]))
            bias = jnp.where(pick, own_bias[layer, h : h + 1, :], peer_bias[layer, h : h + 1, :])
            lines.append(jnp.broadcast_to(bias, (size, bias.shape[1])))
            ends.append(jnp.where(pick, own_out[layer, h], peer_out[layer, h]))
            if both_ref:
                before.append(jnp.where(pick, own_out[layer - 1, h], peer_out[layer - 1, h]))
    table = jnp.concatenate(regroup(blocks, size) + [jnp.concatenate(lines, axis=0).T], axis=1)
    gain = gain_ref[layer : layer + 1, :]
    table = table * jnp.broadcast_to(gain, (gain.shape[1], gain.shape[1])).T[:, :1]
    in_ref[...] = jnp.concatenate(split2(table), axis=0)
    out_ref[...] = jnp.concatenate(split2(jnp.concatenate(ends, axis=0)), axis=0)
    if both_ref:
        before = jnp.concatenate(before, axis=0)
        before = before - jnp.mean(before, axis=-1, keepdims=True)
        both = times_stacked(before, in_ref[...])
        both_ref[0][...] = jnp.concatenate(split2(both), axis=0)


def table_kernel(table_ref, live_ref, out_ref, rows_ref):
    for q in range(OPC):
        rows = table_ref[pl.ds(q, OPC, stride=OPC), :]
        out_ref[q * OPC : (q + 1) * OPC, :] = jnp.concatenate(split2(rows), axis=1)
    sub = lax.broadcasted_iota(jnp.int32, rows_ref.shape, 0)
    live = jnp.zeros(rows_ref.shape, F32)
    for k in range(rows_ref.shape[0]):
        live = jnp.where(sub == k, live_ref[k].astype(F32), live)
    rows_ref[...] = live


def part_kernel(
    heads, own_ref, peer_ref, live_ref, in_0, end_0, in_1, end_1, both_ref, table_ref, out_ref, grad_ref,
    mixed, keys, vals, lines, turns, many, more,
):
    me = lax.axis_index(("row", "head"))
    n = own_ref.shape[0]
    bits = bits_of(n)
    mine_at = reverse(me, bits)
    part = lax.axis_index("br") ^ parity(me, bits)
    straight = (part == 0, part == 1)
    count = n
    rows = own_ref.shape[1] - count - SUBLANES
    total = n * n
    width = live_ref.shape[1]
    in_ref, end_ref = (in_0, in_1), (end_0, end_1)
    heads_wide = end_0.shape[0] // 2
    size = heads_wide // heads

    def taken(start, stop, r, flip):
        slot = mine_at ^ reverse(r, bits)
        mine, other = own_ref[slot, start:stop, :], peer_ref[slot, start:stop, :]
        pick = straight[parity(r, bits)]
        return jnp.where(pick, other, mine) if flip else jnp.where(pick, mine, other)

    def transpose_rows(values, at):
        turn = turns.at[at]
        turn[...] = values
        return jnp.concatenate([turn[pl.ds(j, n, stride=n), :] for j in range(n)], axis=0)

    live = live_ref[...]
    pair_mask = jnp.concatenate([live * live_ref[i : i + 1, :] for i in range(n)], axis=0)
    shift = [(live_ref[k : k + 1, :] - 1.0) * MASK_SHIFT for k in range(n)]

    lefts, rights = [], []
    for flip in (False, True):
        blocks = [taken(0, rows, r, flip) for r in range(n)]
        pieces = regroup(blocks, OPC)
        lefts += [pieces[0], pieces[2]]
        rights += [pieces[1], pieces[3]]
    left, right = jnp.concatenate(lefts, axis=0), jnp.concatenate(rights, axis=0)
    left_high, left_low = split2(left)
    right_high, right_low = split2(right)
    product = dot(
        jnp.concatenate([right_high, right_high, right_low], axis=0),
        jnp.concatenate([left_high, left_low, left_high], axis=0),
        TN,
    )
    per = LANES // OPC
    chunks = []
    for piece in range(n // per):
        mixed[piece] = product[:, piece * LANES : (piece + 1) * LANES]
        lots = []
        for base in range(0, OPC, per):
            lots.append(regroup([mixed[piece, pl.ds(base + g, n, stride=OPC), :] for g in range(per)], OPC))
        chunks += [[lot[g] for lot in lots] for g in range(per)]
    spread = jnp.concatenate([jnp.concatenate(c, axis=1) for c in chunks], axis=0)
    outer = times_beside(spread, table_ref[...])
    seen = jnp.concatenate(
        [own_ref[mine_at ^ reverse(r, bits), rows + count : rows + count + 1, :] for r in range(n)], axis=0
    )
    both = jnp.concatenate([seen * seen[i : i + 1] for i in range(n)], axis=0)
    counts = dot(both.astype(BF16), jnp.ones((LANES, width), BF16))
    pair = jnp.concatenate([taken(rows, rows + count, r, False) for r in range(n)], axis=0)
    cot = jnp.concatenate([taken(rows, rows + count, r, True) for r in range(n)], axis=0)
    pair_one = pair + outer / counts

    same = lax.broadcasted_iota(jnp.int32, (heads_wide, heads_wide), 0) // size
    head = lax.broadcasted_iota(jnp.int32, (heads_wide, heads_wide), 1) // size
    ones = jnp.where(same == head, 1.0, 0.0).astype(BF16)
    ones = jnp.concatenate([ones, ones], axis=0)
    factor = size ** (-0.5)

    def head_sums(values):
        return dot(jnp.concatenate(split2(values), axis=1), ones)

    def block(values, i):
        return values[i * n : (i + 1) * n]

    def forward(layer, entry, own_entry=None, lead=None):
        centred, scale = centre(entry)
        hat = centred * scale

        def project(start, stop):
            weights = in_ref[layer][:, start:stop]
            if lead is None:
                return times_stacked(hat, weights)
            entered, added = lead
            whole = times_stacked(entered, weights) + times_stacked(added, both_ref[:, start:stop])
            return whole * scale

        wide = 2 * heads_wide
        pair_qk = project(0, wide)
        pair_vg = project(wide, 2 * wide)
        bias = project(2 * wide, in_ref[layer].shape[1])
        q, k = pair_qk[:, :heads_wide], pair_qk[:, heads_wide:]
        v, gate = pair_vg[:, :heads_wide], pair_vg[:, heads_wide:]
        q = q * factor
        keys[layer], vals[layer] = k, v
        lines[layer] = bias
        biases = [lines[layer, pl.ds(kk, n, stride=n), :] + shift[kk] for kk in range(n)]
        logits = head_sums(
            jnp.concatenate(
                [block(q, i) * keys[layer, i * n + kk : i * n + kk + 1, :] for i in range(n) for kk in range(n)],
                axis=0,
            )
        )
        probs, attended = [], []
        for i in range(n):
            own = [block(logits, i * n + kk) + biases[kk] for kk in range(n)]
            top = own[0]
            for item in own[1:]:
                top = jnp.maximum(top, item)
            own = [jnp.exp(item - top) for item in own]
            whole = own[0]
            for item in own[1:]:
                whole = whole + item
            inverse = 1.0 / whole
            own = [item * inverse for item in own]
            probs.append(own)
            mix = own[0] * vals[layer, i * n : i * n + 1, :]
            for kk in range(1, n):
                mix = mix + own[kk] * vals[layer, i * n + kk : i * n + kk + 1, :]
            attended.append(mix)
        attended = jnp.concatenate(attended, axis=0)
        opened = jax.nn.sigmoid(gate)
        gated = opened * attended
        if own_entry is not None:
            turns[3] = gated
            gated, entry = turns[3, pl.ds(me, n, stride=n), :], own_entry
            gated = gated * (live * live_ref[pl.ds(me, 1), :])
        else:
            gated = gated * pair_mask
        left = (hat, scale, q, opened, attended, probs)
        return entry + times_stacked(gated, end_ref[layer][...]), left, (centred, gated)

    def row_sums(scratch, start, size):
        whole = scratch[pl.ds(start, size, stride=n), :]
        for j in range(1, n):
            whole = whole + scratch[pl.ds(start + j, size, stride=n), :]
        return whole

    def own_rows(values, at):
        turns[at] = values
        return turns[at, pl.ds(pl.multiple_of(me * n, SUBLANES), n), :]

    def backward(layer, grad, saved, own_only):
        hat, scale, q, opened, attended, probs = saved
        pulled = times_stacked_t(grad * pair_mask, end_ref[layer][...])
        d_att = pulled * opened
        d_gate = d_att * attended * (1.0 - opened)
        d_probs = head_sums(
            jnp.concatenate(
                [block(d_att, i) * vals[layer, i * n + kk : i * n + kk + 1, :] for i in range(n) for kk in range(n)],
                axis=0,
            )
        )
        d_q, d_bias = [], [None] * n
        for i in range(n):
            own = [block(d_probs, i * n + kk) for kk in range(n)]
            both_ = [probs[i][kk] * own[kk] for kk in range(n)]
            mean = both_[0]
            for item in both_[1:]:
                mean = mean + item
            piece = None
            for kk in range(n):
                d_logit = both_[kk] - probs[i][kk] * mean
                at = (i * n + kk) * n
                many[at : at + n, :] = d_logit * block(q, i)
                more[at : at + n, :] = probs[i][kk] * block(d_att, i)
                term = d_logit * keys[layer, i * n + kk : i * n + kk + 1, :]
                piece = term if piece is None else piece + term
                d_bias[kk] = d_logit if d_bias[kk] is None else d_bias[kk] + d_logit
            d_q.append(piece)
        d_q = jnp.concatenate(d_q, axis=0) * factor
        d_bias = jnp.concatenate(d_bias, axis=0) * (1.0 / size)
        start, rows_wanted = 0, total
        if own_only:
            turns[5 + layer] = d_bias
            d_bias = turns[5 + layer, pl.ds(me, n, stride=n), :]
            start, rows_wanted = me * n * n, n
            d_q, d_gate = own_rows(d_q, 4), own_rows(d_gate, 7)
            hat, grad = own_rows(hat, 8), own_rows(grad, 9)
            scale = own_rows(jnp.broadcast_to(scale, (total, width)), 10)
        else:
            d_bias = transpose_rows(d_bias, 5 + layer)
        sums = [row_sums(scratch, start, rows_wanted) for scratch in (many, more)]
        wide = 2 * heads_wide
        d_hat = times_stacked_t(jnp.concatenate([sums[1], d_gate], axis=1), in_ref[layer][:, wide : 2 * wide])
        d_hat = d_hat + times_stacked_t(jnp.concatenate([d_q, sums[0]], axis=1), in_ref[layer][:, :wide])
        d_hat = d_hat + times_stacked_t(d_bias, in_ref[layer][:, 2 * wide :])
        inner = d_hat - jnp.mean(d_hat, axis=-1, keepdims=True)
        inner = inner - hat * jnp.mean(d_hat * hat, axis=-1, keepdims=True)
        return grad + inner * scale

    pair_two, saved_start, (entered, added) = forward(0, pair_one)
    turned_two = transpose_rows(pair_two, 0)
    own_two = turns[0, pl.ds(pl.multiple_of(me * n, SUBLANES), n), :]
    lead = (transpose_rows(entered, 11), transpose_rows(added, 12))
    out_ref[0], saved_end, _ = forward(1, turned_two, own_two, lead)
    grad = backward(1, transpose_rows(cot, 1), saved_end, False)
    grad_ref[0] = backward(0, transpose_rows(grad, 2), saved_start, True)


def spec(space=pltpu.VMEM):
    return pl.BlockSpec(memory_space=space)


def cost(flops):
    return pl.CostEstimate(flops=flops, bytes_accessed=1 << 20, transcendentals=0)


def limit(mebibytes):
    return pltpu.CompilerParams(vmem_limit_bytes=mebibytes << 20)


def bits_of(count):
    return count.bit_length() - 1


def reverse(index, bits):
    back = 0
    for k in range(bits):
        back = back | (((index >> k) & 1) << (bits - 1 - k))
    return back


def parity(index, bits):
    odd = 0
    for k in range(bits):
        odd = odd ^ ((index >> k) & 1)
    return odd


def opposite(count, bit):
    return [(k, k ^ bit) for k in range(count)]


def small_body(*args):
    return gathered(*args)


def gathered(
    pair_acts,
    alignment,
    align_mask,
    residue_mask,
    align_gain,
    outer_in,
    outer_out,
    tri_gain,
    tri_in,
    tri_bias,
    tri_out,
    pair_cotangent,
):
    _, n, width = pair_acts.shape
    seqs = alignment.shape[0]
    layers, _, heads, quad = tri_in.shape
    inner = 2 * heads * (quad // 4)
    swap = opposite(2, 1)
    square = n * n
    bias = jnp.swapaxes(tri_bias, 1, 2)
    firsts = (alignment, outer_in.T, align_gain[None], align_mask.T, pair_acts, pair_cotangent)
    payload = pl.pallas_call(
        project_kernel,
        out_shape=jax.ShapeDtypeStruct((seqs // 2 + n + SUBLANES, LANES), F32),
        in_specs=[spec(pltpu.HBM)] * len(firsts),
        out_specs=spec(),
        scratch_shapes=[pltpu.VMEM(v.shape, v.dtype) for v in firsts]
        + [pltpu.SemaphoreType.DMA((len(firsts),))],
        compiler_params=limit(2),
        name="project",
    )(*[pltpu.with_memory_space_constraint(v, pltpu.HBM) for v in firsts])
    table, live_rows = pl.pallas_call(
        table_kernel,
        out_shape=(
            jax.ShapeDtypeStruct((outer_out.shape[0], 2 * width), BF16),
            jax.ShapeDtypeStruct((n, width), F32),
        ),
        in_specs=[spec(), spec(pltpu.SMEM)],
        out_specs=(spec(), spec()),
        compiler_params=limit(4),
        cost_estimate=cost(1 << 22),
        name="table",
    )(outer_out, residue_mask)
    peers = []
    for value in (tri_in, bias, tri_out):
        peers.append(lax.ppermute(value, "br", swap))
    weights = []
    for layer in range(layers):
        weights += pl.pallas_call(
            functools.partial(weights_kernel, layer),
            out_shape=(
                jax.ShapeDtypeStruct((2 * width, 5 * inner), BF16),
                jax.ShapeDtypeStruct((2 * inner, width), BF16),
            )
            + (jax.ShapeDtypeStruct((2 * inner, 5 * inner), BF16),) * min(layer, 1),
            in_specs=[spec()] * 7,
            out_specs=(spec(),) * (2 + min(layer, 1)),
            compiler_params=limit(4),
            cost_estimate=cost(1 << 22),
        )(tri_gain, tri_in, peers[0], bias, peers[1], tri_out, peers[2])
    held = payload[None]
    for at in range(bits_of(n)):
        pairs = opposite(2 * n, (n >> at) | 1)
        got = lax.ppermute(held, ("row", "head", "br"), pairs)
        held = jnp.concatenate([held, got], axis=0)
    other = lax.ppermute(held, "br", swap)
    shape = jax.ShapeDtypeStruct((1, n, width), F32)
    return pl.pallas_call(
        functools.partial(part_kernel, 2 * heads),
        out_shape=(shape, shape),
        in_specs=[spec()] * 9,
        out_specs=(spec(), spec()),
        scratch_shapes=[
            pltpu.VMEM((n * OPC // LANES, n * OPC, LANES), F32),
            pltpu.VMEM((layers, square, inner), F32),
            pltpu.VMEM((layers, square, inner), F32),
            pltpu.VMEM((layers, square, inner), F32),
            pltpu.VMEM((11 + layers, square, width), F32),
            pltpu.VMEM((square * n, inner), F32),
            pltpu.VMEM((square * n, inner), F32),
        ],
        compiler_params=limit(8),
        name="part",
    )(held, other, live_rows, *weights, table)


def is_small(mesh, residues, seqs, width, inner):
    group = mesh.shape["row"] * mesh.shape["head"]
    powers = all(mesh.shape[a] & (mesh.shape[a] - 1) == 0 for a in ("row", "head"))
    return (
        powers
        and mesh.shape["br"] == 2
        and residues == group == SUBLANES
        and seqs % (2 * 2 * SUBLANES) == 0
        and seqs <= LANES
        and 4 * OPC == width == inner == LANES
    )


def solution(mesh):
    in_specs = (
        P(("grp", "row", "head"), None, None),
        P(("grp", "br"), ("row", "head"), None),
        P("grp", ("row", "head")),
        P("grp"),
        P(),
        P(),
        P(),
        P(),
        P(None, None, "br", None),
        P(None, None, "br"),
        P(None, "br", None, None),
        P(("grp", "row", "head"), None, None),
    )
    out_specs = (P(("grp", "row", "head"), None, None), P(("grp", "row", "head"), None, None))

    def mapped(*args):
        residues, seqs = args[0].shape[1], args[1].shape[0] // mesh.shape["grp"]
        width, inner = args[0].shape[2], args[10].shape[1] * args[10].shape[2]
        small = is_small(mesh, residues, seqs, width, inner)
        chosen = small_body if small else body
        step = jax.shard_map(chosen, mesh=mesh, in_specs=in_specs, out_specs=out_specs, check_vma=False)
        return step(*args)

    return mapped
```

```python
import functools

import jax
import jax.numpy as jnp
from jax import lax
from jax.experimental import pallas as pl
from jax.experimental.pallas import tpu as pltpu
from jax.sharding import PartitionSpec as P


OPC = 32


PRECISE = lax.Precision.HIGHEST
EPSILON = 1e-05
MASK_SHIFT = 1000000000.0


def normalize(values, scales):
    average = jnp.mean(values, axis=-1, keepdims=True)
    centred = values - average
    spread = jnp.mean(centred * centred, axis=-1, keepdims=True)
    return centred * lax.rsqrt(spread + EPSILON) * scales


def core_total(values):
    return lax.psum(values, "br")


def reorient(values):
    turned = jnp.swapaxes(values, 0, 1)
    return lax.all_to_all(turned, ("row", "head"), split_axis=0, concat_axis=1, tiled=True)


def prepare(values, scales, weight_in, weight_bias):
    normed = normalize(values, scales)
    projected = jnp.einsum("ijc,chd->ijhd", normed, weight_in, precision=PRECISE)
    bias_local = jnp.einsum("jkc,ch->hjk", normed, weight_bias, precision=PRECISE)
    return (projected, bias_local)


def attend(projected, bias_full, key_shift, weight_out):
    head_size = projected.shape[-1] // 4
    queries = projected[..., :head_size]
    key_proj = projected[..., head_size : 2 * head_size]
    value_proj = projected[..., 2 * head_size : 3 * head_size]
    gating = projected[..., 3 * head_size :]
    logits = jnp.einsum("ijhd,ikhd->ihjk", queries, key_proj, precision=PRECISE) * head_size ** (
        -0.5
    )
    logits = logits + bias_full[None] + key_shift
    attention = jax.nn.softmax(logits, axis=-1)
    attended = jnp.einsum("ihjk,ikhd->ijhd", attention, value_proj, precision=PRECISE)
    gated_out = jax.nn.sigmoid(gating) * attended
    return jnp.einsum("ijhd,hdc->ijc", gated_out, weight_out, precision=PRECISE)


def tri_forward(rows_in, scales, weight_in, weight_bias, weight_out, key_shift, pair_mask):

    def local_prep(values):
        return prepare(values, scales, weight_in, weight_bias)

    (projected, bias_local), pull_prep = jax.vjp(local_prep, rows_in)
    bias_full = lax.all_gather(bias_local, ("row", "head"), axis=1, tiled=True)

    def local_attend(proj_in, bias_in):
        return attend(proj_in, bias_in, key_shift, weight_out)

    partial_out, pull_attend = jax.vjp(local_attend, projected, bias_full)
    total_out = core_total(partial_out)
    return (rows_in + total_out * pair_mask, (pull_prep, pull_attend))


def tri_backward(grad_out, saved, pair_mask):
    pull_prep, pull_attend = saved
    grad_proj, grad_bias = pull_attend(grad_out * pair_mask)
    grad_local = lax.psum_scatter(grad_bias, ("row", "head"), scatter_dimension=1, tiled=True)
    (grad_rows,) = pull_prep((grad_proj, grad_local))
    return grad_out + core_total(grad_rows)


def body(
    pair_acts,
    alignment,
    align_mask,
    residue_mask,
    align_gain,
    outer_in,
    outer_out,
    tri_gain,
    tri_in,
    tri_bias,
    tri_out,
    pair_cotangent,
):
    row_count = pair_acts.shape[0]
    live = residue_mask.astype(jnp.float32)
    key_shift = (live - 1.0) * MASK_SHIFT
    row_live = lax.dynamic_slice_in_dim(
        live, lax.axis_index(("row", "head")) * row_count, row_count, 0
    )
    pair_mask = row_live[:, None, None] * live[None, :, None]
    seq_count = alignment.shape[0]
    mask_all = align_mask.astype(jnp.float32)
    mask_own = lax.dynamic_slice_in_dim(mask_all, lax.axis_index("br") * seq_count, seq_count, 0)
    normed = normalize(alignment, align_gain)
    projected = jnp.einsum("snc,ck->snk", normed, outer_in, precision=PRECISE)
    left_part = projected[..., :OPC] * mask_own[..., None]
    right_part = jnp.swapaxes(projected[..., OPC:] * mask_own[..., None], 1, 2)
    right_all, mask_cols = (
        lax.all_gather(right_part, ("row", "head"), axis=2, tiled=True),
        lax.all_gather(mask_all, ("row", "head"), axis=1, tiled=True),
    )
    counts = jnp.einsum("si,sj->ij", mask_all, mask_cols, precision=PRECISE)
    table = outer_out.reshape(OPC, OPC, outer_out.shape[-1])
    mixed_left = jnp.einsum("sip,pqc->siqc", left_part, table, precision=PRECISE)
    partial_outer = jnp.einsum("siqc,sqj->ijc", mixed_left, right_all, precision=PRECISE)
    outer_sum = core_total(partial_outer)
    pair_one = pair_acts + outer_sum / counts[..., None]
    pair_two, saved_start = tri_forward(
        pair_one, tri_gain[0], tri_in[0], tri_bias[0], tri_out[0], key_shift, pair_mask
    )
    turned_two = reorient(pair_two)
    turned_three, saved_end = tri_forward(
        turned_two, tri_gain[1], tri_in[1], tri_bias[1], tri_out[1], key_shift, pair_mask
    )
    pair_out = reorient(turned_three)
    grad_turned = reorient(pair_cotangent)
    grad_turned = tri_backward(grad_turned, saved_end, pair_mask)
    grad_two = reorient(grad_turned)
    pair_grad = tri_backward(grad_two, saved_start, pair_mask)
    return (pair_out, pair_grad)


F32 = jnp.float32
BF16 = jnp.bfloat16
LANES = 128
SUBLANES = 8
NN = (((1,), (0,)), ((), ()))
NT = (((1,), (1,)), ((), ()))
TN = (((0,), (0,)), ((), ()))


def split2(values):
    high = values.astype(BF16)
    return high, (values - high.astype(F32)).astype(BF16)


def dot(left, right, dims=NN):
    return lax.dot_general(left, right, dims, preferred_element_type=F32)


def times_stacked(values, stacked):
    high, low = split2(values)
    depth = stacked.shape[0] // 2
    return dot(jnp.concatenate([high, high], axis=1), stacked) + dot(low, stacked[:depth])


def fold(product, rows, columns):
    return product[:rows, :columns] + product[:rows, columns:] + product[rows:, :columns]


def times_stacked_t(values, stacked):
    high, low = split2(values)
    product = dot(jnp.concatenate([high, low], axis=0), stacked, NT)
    return fold(product, values.shape[0], stacked.shape[0] // 2)


def times_beside(values, beside):
    high, low = split2(values)
    product = dot(jnp.concatenate([high, low], axis=0), beside)
    return fold(product, values.shape[0], beside.shape[1] // 2)


def centre(values):
    average = jnp.mean(values, axis=-1, keepdims=True)
    centred = values - average
    scale = lax.rsqrt(jnp.mean(centred * centred, axis=-1, keepdims=True) + EPSILON)
    return centred, scale


def regroup(blocks, width):
    groups = blocks[0].shape[1] // width
    return [
        jnp.concatenate([block[:, g * width : (g + 1) * width] for block in blocks], axis=1)
        for g in range(groups)
    ]


def project_kernel(*refs):
    count = (len(refs) - 2) // 2
    sources, out_ref, held, sems = refs[:count], refs[count], refs[count + 1 : -1], refs[-1]
    copies = [
        pltpu.make_async_copy(source, place, sems.at[k])
        for k, (source, place) in enumerate(zip(sources, held))
    ]
    for copy in copies:
        copy.start()
    align_ref, proj_ref, gain_ref, mask_ref, pair_ref, cot_ref = held
    part = lax.axis_index("br")
    seqs, _, width = align_ref.shape
    rows = seqs // 2
    copies[0].wait()
    centred, scale = centre(jnp.reshape(align_ref[...], (seqs, width)))
    normed = centred * scale
    copies[1].wait()
    stacked = jnp.concatenate(split2(proj_ref[...]), axis=0)
    copies[2].wait()
    projected = times_stacked_t(normed * gain_ref[...], stacked)
    copies[3].wait()
    line = mask_ref[...].astype(F32)
    sequence = lax.broadcasted_iota(jnp.int32, (seqs, line.shape[1]), 0) + part * seqs
    lane = lax.broadcasted_iota(jnp.int32, (seqs, line.shape[1]), 1)
    own = jnp.sum(jnp.where(sequence == lane, line, 0.0), axis=1, keepdims=True)
    rest = jnp.zeros((1, LANES - line.shape[1]), F32)
    line = jnp.concatenate([line, rest], axis=1)
    count = pair_ref.shape[1]
    out_ref[rows + count :, :] = jnp.broadcast_to(line, (SUBLANES, LANES))
    copies[4].wait()
    copies[5].wait()
    out_ref[rows : rows + count, :] = jnp.where(part == 0, pair_ref[0], cot_ref[0])
    projected = projected * own
    out_ref[0:rows, :] = jnp.concatenate([projected[:rows], projected[rows:]], axis=1)


def weights_kernel(layer, gain_ref, own_in, peer_in, own_bias, peer_bias, own_out, peer_out, in_ref, out_ref, *both_ref):
    first = lax.axis_index("br") == 0
    heads, width = own_in.shape[2:]
    size = width // 4
    blocks, lines, ends, before = [], [], [], []
    for half in range(2):
        pick = first if half == 0 else jnp.logical_not(first)
        for h in range(heads):
            blocks.append(jnp.where(pick, own_in[layer, :, h, :], peer_in[layer, :, h, :]))
            bias = jnp.where(pick, own_bias[layer, h : h + 1, :], peer_bias[layer, h : h + 1, :])
            lines.append(jnp.broadcast_to(bias, (size, bias.shape[1])))
            ends.append(jnp.where(pick, own_out[layer, h], peer_out[layer, h]))
            if both_ref:
                before.append(jnp.where(pick, own_out[layer - 1, h], peer_out[layer - 1, h]))
    table = jnp.concatenate(regroup(blocks, size) + [jnp.concatenate(lines, axis=0).T], axis=1)
    gain = gain_ref[layer : layer + 1, :]
    table = table * jnp.broadcast_to(gain, (gain.shape[1], gain.shape[1])).T[:, :1]
    in_ref[...] = jnp.concatenate(split2(table), axis=0)
    out_ref[...] = jnp.concatenate(split2(jnp.concatenate(ends, axis=0)), axis=0)
    if both_ref:
        before = jnp.concatenate(before, axis=0)
        before = before - jnp.mean(before, axis=-1, keepdims=True)
        both = times_stacked(before, in_ref[...])
        both_ref[0][...] = jnp.concatenate(split2(both), axis=0)


def table_kernel(table_ref, live_ref, out_ref, rows_ref):
    for q in range(OPC):
        rows = table_ref[pl.ds(q, OPC, stride=OPC), :]
        out_ref[q * OPC : (q + 1) * OPC, :] = jnp.concatenate(split2(rows), axis=1)
    sub = lax.broadcasted_iota(jnp.int32, rows_ref.shape, 0)
    live = jnp.zeros(rows_ref.shape, F32)
    for k in range(rows_ref.shape[0]):
        live = jnp.where(sub == k, live_ref[k].astype(F32), live)
    rows_ref[...] = live


def part_kernel(
    heads, own_ref, peer_ref, live_ref, in_0, end_0, in_1, end_1, both_ref, table_ref, out_ref, grad_ref,
    mixed, keys, vals, lines, turns, many, more,
):
    me = lax.axis_index(("row", "head"))
    n = own_ref.shape[0]
    bits = bits_of(n)
    mine_at = reverse(me, bits)
    part = lax.axis_index("br") ^ parity(me, bits)
    straight = (part == 0, part == 1)
    count = n
    rows = own_ref.shape[1] - count - SUBLANES
    total = n * n
    width = live_ref.shape[1]
    in_ref, end_ref = (in_0, in_1), (end_0, end_1)
    heads_wide = end_0.shape[0] // 2
    size = heads_wide // heads

    def taken(start, stop, r, flip):
        slot = mine_at ^ reverse(r, bits)
        mine, other = own_ref[slot, start:stop, :], peer_ref[slot, start:stop, :]
        pick = straight[parity(r, bits)]
        return jnp.where(pick, other, mine) if flip else jnp.where(pick, mine, other)

    def transpose_rows(values, at):
        turn = turns.at[at]
        turn[...] = values
        return jnp.concatenate([turn[pl.ds(j, n, stride=n), :] for j in range(n)], axis=0)

    live = live_ref[...]
    pair_mask = jnp.concatenate([live * live_ref[i : i + 1, :] for i in range(n)], axis=0)
    shift = [(live_ref[k : k + 1, :] - 1.0) * MASK_SHIFT for k in range(n)]

    lefts, rights = [], []
    for flip in (False, True):
        blocks = [taken(0, rows, r, flip) for r in range(n)]
        pieces = regroup(blocks, OPC)
        lefts += [pieces[0], pieces[2]]
        rights += [pieces[1], pieces[3]]
    left, right = jnp.concatenate(lefts, axis=0), jnp.concatenate(rights, axis=0)
    left_high, left_low = split2(left)
    right_high, right_low = split2(right)
    product = dot(
        jnp.concatenate([right_high, right_high, right_low], axis=0),
        jnp.concatenate([left_high, left_low, left_high], axis=0),
        TN,
    )
    per = LANES // OPC
    chunks = []
    for piece in range(n // per):
        mixed[piece] = product[:, piece * LANES : (piece + 1) * LANES]
        lots = []
        for base in range(0, OPC, per):
            lots.append(regroup([mixed[piece, pl.ds(base + g, n, stride=OPC), :] for g in range(per)], OPC))
        chunks += [[lot[g] for lot in lots] for g in range(per)]
    spread = jnp.concatenate([jnp.concatenate(c, axis=1) for c in chunks], axis=0)
    outer = times_beside(spread, table_ref[...])
    seen = jnp.concatenate(
        [own_ref[mine_at ^ reverse(r, bits), rows + count : rows + count + 1, :] for r in range(n)], axis=0
    )
    both = jnp.concatenate([seen * seen[i : i + 1] for i in range(n)], axis=0)
    counts = dot(both.astype(BF16), jnp.ones((LANES, width), BF16))
    pair = jnp.concatenate([taken(rows, rows + count, r, False) for r in range(n)], axis=0)
    cot = jnp.concatenate([taken(rows, rows + count, r, True) for r in range(n)], axis=0)
    pair_one = pair + outer / counts

    same = lax.broadcasted_iota(jnp.int32, (heads_wide, heads_wide), 0) // size
    head = lax.broadcasted_iota(jnp.int32, (heads_wide, heads_wide), 1) // size
    ones = jnp.where(same == head, 1.0, 0.0).astype(BF16)
    ones = jnp.concatenate([ones, ones], axis=0)
    factor = size ** (-0.5)

    def head_sums(values):
        return dot(jnp.concatenate(split2(values), axis=1), ones)

    def block(values, i):
        return values[i * n : (i + 1) * n]

    def forward(layer, entry, own_entry=None, lead=None):
        centred, scale = centre(entry)
        hat = centred * scale

        def project(start, stop):
            weights = in_ref[layer][:, start:stop]
            if lead is None:
                return times_stacked(hat, weights)
            entered, added = lead
            whole = times_stacked(entered, weights) + times_stacked(added, both_ref[:, start:stop])
            return whole * scale

        wide = 2 * heads_wide
        pair_qk = project(0, wide)
        pair_vg = project(wide, 2 * wide)
        bias = project(2 * wide, in_ref[layer].shape[1])
        q, k = pair_qk[:, :heads_wide], pair_qk[:, heads_wide:]
        v, gate = pair_vg[:, :heads_wide], pair_vg[:, heads_wide:]
        q = q * factor
        keys[layer], vals[layer] = k, v
        lines[layer] = bias
        biases = [lines[layer, pl.ds(kk, n, stride=n), :] + shift[kk] for kk in range(n)]
        logits = head_sums(
            jnp.concatenate(
                [block(q, i) * keys[layer, i * n + kk : i * n + kk + 1, :] for i in range(n) for kk in range(n)],
                axis=0,
            )
        )
        probs, attended = [], []
        for i in range(n):
            own = [block(logits, i * n + kk) + biases[kk] for kk in range(n)]
            top = own[0]
            for item in own[1:]:
                top = jnp.maximum(top, item)
            own = [jnp.exp(item - top) for item in own]
            whole = own[0]
            for item in own[1:]:
                whole = whole + item
            inverse = 1.0 / whole
            own = [item * inverse for item in own]
            probs.append(own)
            mix = own[0] * vals[layer, i * n : i * n + 1, :]
            for kk in range(1, n):
                mix = mix + own[kk] * vals[layer, i * n + kk : i * n + kk + 1, :]
            attended.append(mix)
        attended = jnp.concatenate(attended, axis=0)
        opened = jax.nn.sigmoid(gate)
        gated = opened * attended
        if own_entry is not None:
            turns[3] = gated
            gated, entry = turns[3, pl.ds(me, n, stride=n), :], own_entry
            gated = gated * (live * live_ref[pl.ds(me, 1), :])
        else:
            gated = gated * pair_mask
        left = (hat, scale, q, opened, attended, probs)
        return entry + times_stacked(gated, end_ref[layer][...]), left, (centred, gated)

    def row_sums(scratch, start, size):
        whole = scratch[pl.ds(start, size, stride=n), :]
        for j in range(1, n):
            whole = whole + scratch[pl.ds(start + j, size, stride=n), :]
        return whole

    def own_rows(values, at):
        turns[at] = values
        return turns[at, pl.ds(pl.multiple_of(me * n, SUBLANES), n), :]

    def backward(layer, grad, saved, own_only):
        hat, scale, q, opened, attended, probs = saved
        pulled = times_stacked_t(grad * pair_mask, end_ref[layer][...])
        d_att = pulled * opened
        d_gate = d_att * attended * (1.0 - opened)
        d_probs = head_sums(
            jnp.concatenate(
                [block(d_att, i) * vals[layer, i * n + kk : i * n + kk + 1, :] for i in range(n) for kk in range(n)],
                axis=0,
            )
        )
        d_q, d_bias = [], [None] * n
        for i in range(n):
            own = [block(d_probs, i * n + kk) for kk in range(n)]
            both_ = [probs[i][kk] * own[kk] for kk in range(n)]
            mean = both_[0]
            for item in both_[1:]:
                mean = mean + item
            piece = None
            for kk in range(n):
                d_logit = both_[kk] - probs[i][kk] * mean
                at = (i * n + kk) * n
                many[at : at + n, :] = d_logit * block(q, i)
                more[at : at + n, :] = probs[i][kk] * block(d_att, i)
                term = d_logit * keys[layer, i * n + kk : i * n + kk + 1, :]
                piece = term if piece is None else piece + term
                d_bias[kk] = d_logit if d_bias[kk] is None else d_bias[kk] + d_logit
            d_q.append(piece)
        d_q = jnp.concatenate(d_q, axis=0) * factor
        d_bias = jnp.concatenate(d_bias, axis=0) * (1.0 / size)
        start, rows_wanted = 0, total
        if own_only:
            turns[5 + layer] = d_bias
            d_bias = turns[5 + layer, pl.ds(me, n, stride=n), :]
            start, rows_wanted = me * n * n, n
            d_q, d_gate = own_rows(d_q, 4), own_rows(d_gate, 7)
            hat, grad = own_rows(hat, 8), own_rows(grad, 9)
            scale = own_rows(jnp.broadcast_to(scale, (total, width)), 10)
        else:
            d_bias = transpose_rows(d_bias, 5 + layer)
        sums = [row_sums(scratch, start, rows_wanted) for scratch in (many, more)]
        wide = 2 * heads_wide
        d_hat = times_stacked_t(jnp.concatenate([sums[1], d_gate], axis=1), in_ref[layer][:, wide : 2 * wide])
        d_hat = d_hat + times_stacked_t(jnp.concatenate([d_q, sums[0]], axis=1), in_ref[layer][:, :wide])
        d_hat = d_hat + times_stacked_t(d_bias, in_ref[layer][:, 2 * wide :])
        inner = d_hat - jnp.mean(d_hat, axis=-1, keepdims=True)
        inner = inner - hat * jnp.mean(d_hat * hat, axis=-1, keepdims=True)
        return grad + inner * scale

    pair_two, saved_start, (entered, added) = forward(0, pair_one)
    turned_two = transpose_rows(pair_two, 0)
    own_two = turns[0, pl.ds(pl.multiple_of(me * n, SUBLANES), n), :]
    lead = (transpose_rows(entered, 11), transpose_rows(added, 12))
    out_ref[0], saved_end, _ = forward(1, turned_two, own_two, lead)
    grad = backward(1, transpose_rows(cot, 1), saved_end, False)
    grad_ref[0] = backward(0, transpose_rows(grad, 2), saved_start, True)


def spec(space=pltpu.VMEM):
    return pl.BlockSpec(memory_space=space)


def cost(flops):
    return pl.CostEstimate(flops=flops, bytes_accessed=1 << 20, transcendentals=0)


def limit(mebibytes):
    return pltpu.CompilerParams(vmem_limit_bytes=mebibytes << 20)


def bits_of(count):
    return count.bit_length() - 1


def step_bits(bits):
    return [bits - 1, *range(bits - 1)]


def reverse(index, bits):
    slot = 0
    for k, bit in enumerate(step_bits(bits)):
        slot = slot | (((index >> bit) & 1) << k)
    return slot


def parity(index, bits):
    odd = 0
    for k in range(bits):
        odd = odd ^ ((index >> k) & 1)
    return odd


def opposite(count, bit):
    return [(k, k ^ bit) for k in range(count)]


def small_body(*args):
    return gathered(*args)


def gathered(
    pair_acts,
    alignment,
    align_mask,
    residue_mask,
    align_gain,
    outer_in,
    outer_out,
    tri_gain,
    tri_in,
    tri_bias,
    tri_out,
    pair_cotangent,
):
    _, n, width = pair_acts.shape
    seqs = alignment.shape[0]
    layers, _, heads, quad = tri_in.shape
    inner = 2 * heads * (quad // 4)
    swap = opposite(2, 1)
    square = n * n
    bias = jnp.swapaxes(tri_bias, 1, 2)
    firsts = (alignment, outer_in.T, align_gain[None], align_mask.T, pair_acts, pair_cotangent)
    payload = pl.pallas_call(
        project_kernel,
        out_shape=jax.ShapeDtypeStruct((seqs // 2 + n + SUBLANES, LANES), F32),
        in_specs=[spec(pltpu.HBM)] * len(firsts),
        out_specs=spec(),
        scratch_shapes=[pltpu.VMEM(v.shape, v.dtype) for v in firsts]
        + [pltpu.SemaphoreType.DMA((len(firsts),))],
        compiler_params=limit(2),
        name="project",
    )(*[pltpu.with_memory_space_constraint(v, pltpu.HBM) for v in firsts])
    table, live_rows = pl.pallas_call(
        table_kernel,
        out_shape=(
            jax.ShapeDtypeStruct((outer_out.shape[0], 2 * width), BF16),
            jax.ShapeDtypeStruct((n, width), F32),
        ),
        in_specs=[spec(), spec(pltpu.SMEM)],
        out_specs=(spec(), spec()),
        compiler_params=limit(4),
        cost_estimate=cost(1 << 22),
        name="table",
    )(outer_out, residue_mask)
    peers = []
    for value in (tri_in, bias, tri_out):
        peers.append(lax.ppermute(value, "br", swap))
    weights = []
    for layer in range(layers):
        weights += pl.pallas_call(
            functools.partial(weights_kernel, layer),
            out_shape=(
                jax.ShapeDtypeStruct((2 * width, 5 * inner), BF16),
                jax.ShapeDtypeStruct((2 * inner, width), BF16),
            )
            + (jax.ShapeDtypeStruct((2 * inner, 5 * inner), BF16),) * min(layer, 1),
            in_specs=[spec()] * 7,
            out_specs=(spec(),) * (2 + min(layer, 1)),
            compiler_params=limit(4),
            cost_estimate=cost(1 << 22),
        )(tri_gain, tri_in, peers[0], bias, peers[1], tri_out, peers[2])
    held = payload[None]
    for bit in step_bits(bits_of(n)):
        pairs = opposite(2 * n, (2 << bit) | 1)
        got = lax.ppermute(held, ("row", "head", "br"), pairs)
        held = jnp.concatenate([held, got], axis=0)
    other = lax.ppermute(held, "br", swap)
    shape = jax.ShapeDtypeStruct((1, n, width), F32)
    return pl.pallas_call(
        functools.partial(part_kernel, 2 * heads),
        out_shape=(shape, shape),
        in_specs=[spec()] * 9,
        out_specs=(spec(), spec()),
        scratch_shapes=[
            pltpu.VMEM((n * OPC // LANES, n * OPC, LANES), F32),
            pltpu.VMEM((layers, square, inner), F32),
            pltpu.VMEM((layers, square, inner), F32),
            pltpu.VMEM((layers, square, inner), F32),
            pltpu.VMEM((11 + layers, square, width), F32),
            pltpu.VMEM((square * n, inner), F32),
            pltpu.VMEM((square * n, inner), F32),
        ],
        compiler_params=limit(8),
        name="part",
    )(held, other, live_rows, *weights, table)


def is_small(mesh, residues, seqs, width, inner):
    group = mesh.shape["row"] * mesh.shape["head"]
    powers = all(mesh.shape[a] & (mesh.shape[a] - 1) == 0 for a in ("row", "head"))
    return (
        powers
        and mesh.shape["br"] == 2
        and residues == group == SUBLANES
        and seqs % (2 * 2 * SUBLANES) == 0
        and seqs <= LANES
        and 4 * OPC == width == inner == LANES
    )


def solution(mesh):
    in_specs = (
        P(("grp", "row", "head"), None, None),
        P(("grp", "br"), ("row", "head"), None),
        P("grp", ("row", "head")),
        P("grp"),
        P(),
        P(),
        P(),
        P(),
        P(None, None, "br", None),
        P(None, None, "br"),
        P(None, "br", None, None),
        P(("grp", "row", "head"), None, None),
    )
    out_specs = (P(("grp", "row", "head"), None, None), P(("grp", "row", "head"), None, None))

    def mapped(*args):
        residues, seqs = args[0].shape[1], args[1].shape[0] // mesh.shape["grp"]
        width, inner = args[0].shape[2], args[10].shape[1] * args[10].shape[2]
        small = is_small(mesh, residues, seqs, width, inner)
        chosen = small_body if small else body
        step = jax.shard_map(chosen, mesh=mesh, in_specs=in_specs, out_specs=out_specs, check_vma=False)
        return step(*args)

    return mapped
```
